32 devices in a mesh: data: 1 (over z), tp2: 4 (over y), tp: 8 (over x, core).
Axes of the slice: x: 4, y: 4, z: 1, core: 2. Of those that a mesh axis runs over, the one named last changes fastest.
The devices are a block of a 4x4x8 slice.
Arguments:
- x_resid: bfloat16 [4096, 8192], P(('data', 'tp'), 'tp2')
- ln_scale: float32 [8192], P('tp2')
- w_in: bfloat16 [8192, 28672], P('tp2', 'tp')
- w_out: bfloat16 [28672, 8192], P('tp', 'tp2')
Outputs:
- output: bfloat16 [4096, 8192], P(('data', 'tp'), 'tp2')
All inputs are finite; a program needn't handle non-finite values.
Results may differ from the reference program's by a relative error of at most 0.00132.
Values are sent between devices in bfloat16 or wider.
A program may use at most 768 MiB of HBM per device.

```python
import jax
import jax.numpy as jnp
from jax import lax
import math

SEQ_LEN = 4096
MODEL_DIM = 8192
FFN_DIM = 28672
LN_EPS = 1e-6
ROW_BLOCK = min(SEQ_LEN, 512)


def setup_inputs(seed: int = 0, part: int = 0) -> dict:
    base_key = jax.random.key(seed)
    key_gamma, key_in, key_out, key_act = jax.random.split(base_key, 4)
    key_act = jax.random.fold_in(key_act, part)
    key_noise, key_rshift, key_rscale, key_phase, key_amp = jax.random.split(key_act, 5)
    col_pos = jnp.arange(MODEL_DIM, dtype=jnp.float32) * (2.0 * math.pi / MODEL_DIM)
    phase_vals = jax.random.uniform(key_phase, (4,), jnp.float32, minval=0.0, maxval=2.0 * math.pi)
    amp_vals = jax.random.uniform(key_amp, (4,), jnp.float32, minval=0.3, maxval=0.7)
    col_scale = jnp.exp(amp_vals[0] * jnp.cos(col_pos + phase_vals[0]) + amp_vals[1] * jnp.cos(2.0 * col_pos + phase_vals[1]))
    col_shift = 1.5 * amp_vals[2] * jnp.sin(col_pos + phase_vals[2]) + amp_vals[3] * jnp.sin(3.0 * col_pos + phase_vals[3])
    row_shift = jax.random.normal(key_rshift, (SEQ_LEN, 1), jnp.float32)
    row_scale = jnp.exp(0.3 * jax.random.normal(key_rscale, (SEQ_LEN, 1), jnp.float32))
    noise_val = jax.random.normal(key_noise, (SEQ_LEN, MODEL_DIM), jnp.float32)
    x_resid = row_scale * (noise_val * col_scale + row_shift * col_shift)
    ln_scale = 1.0 + 0.4 * jax.random.normal(key_gamma, (MODEL_DIM,), jnp.float32)
    w_in = jax.random.normal(key_in, (MODEL_DIM, FFN_DIM), jnp.float32) * (MODEL_DIM ** -0.5)
    w_out = jax.random.normal(key_out, (FFN_DIM, MODEL_DIM), jnp.float32) * (1.5 * FFN_DIM ** -0.5)
    return {"x_resid": x_resid.astype(jnp.bfloat16), "ln_scale": ln_scale, "w_in": w_in.astype(jnp.bfloat16), "w_out": w_out.astype(jnp.bfloat16)}


def reference(x_resid, ln_scale, w_in, w_out):
    row_blocks = x_resid.reshape(SEQ_LEN // ROW_BLOCK, ROW_BLOCK, MODEL_DIM)

    def one_block(x_blk):
        x_f32 = x_blk.astype(jnp.float32)
        row_mean = jnp.mean(x_f32, axis=-1, keepdims=True)
        centered = x_f32 - row_mean
        row_var = jnp.mean(centered * centered, axis=-1, keepdims=True)
        x_norm = (centered * lax.rsqrt(row_var + LN_EPS) * ln_scale).astype(jnp.bfloat16)
        pre_act = jnp.dot(x_norm, w_in, preferred_element_type=jnp.float32)
        hidden = jax.nn.gelu(pre_act, approximate=True).astype(jnp.bfloat16)
        mlp_out = jnp.dot(hidden, w_out, preferred_element_type=jnp.float32)
        return (x_f32 + mlp_out).astype(jnp.bfloat16)

    return lax.map(one_block, row_blocks).reshape(SEQ_LEN, MODEL_DIM)
```

```python
import functools

import jax
import jax.numpy as jnp
from jax import lax
from jax.experimental import pallas as pl
from jax.experimental.pallas import tpu as pltpu
from jax.sharding import PartitionSpec as P

LN_EPS = 1e-6
RING = 4
TICKS = 16
AHEAD = 4
HSLOTS = 5
MESH = pl.DeviceIdType.MESH
BF16, F32 = jnp.bfloat16, jnp.float32


def kernel(dims, x_ref, g_ref, w1_ref, w2_ref, y_ref, raw_ref, xall_ref, w1v, w2v, xv, hv, sv, pv, pr, hr, tr, xr, gv, lr, ln,
           g_s, g_r, raw_s, raw_r, w1_s, w1_r, x_s, x_r, d_s, d_r, h_s, h_r, q_s, p_s, p_r, f_s, f_r, t_s, t_r, l_s, xl_s, o_s):
    T, KB, NS, DB, r, M = dims
    J = TICKS
    K = RING * KB
    half = r // 2
    d = lax.axis_index("data")
    y = lax.axis_index("tp2")
    tp = lax.axis_index("tp")
    x, c = tp // 2, tp % 2
    yp, yo, ym = (y + 1) % RING, (y + 2) % RING, (y + 3) % RING
    xp, xo, xm = (x + 1) % RING, (x + 2) % RING, (x + 3) % RING
    to_yp, to_ym, to_yo = (d, yp, tp), (d, ym, tp), (d, yo, tp)
    to_xp, to_xm = (d, y, xp * 2 + c), (d, y, xm * 2 + c)
    to_pt = (d, y, x * 2 + 1 - c)

    def rc(src, dst, ss, rs, dev):
        return pltpu.make_async_remote_copy(src_ref=src, dst_ref=dst, send_sem=ss, recv_sem=rs, device_id=dev, device_id_type=MESH)

    def loop(lo, hi, f):
        def body(i, carry):
            f(i)
            return carry
        lax.fori_loop(lo, hi, body, 0)

    barrier = pltpu.get_barrier_semaphore()
    for dev in (to_yp, to_ym, to_yo, to_xp, to_xm, to_pt):
        pl.semaphore_signal(barrier, inc=1, device_id=dev, device_id_type=MESH)
    pl.semaphore_wait(barrier, 6)

    def raw_own(j, dev, i, k):
        rows = pl.ds(pl.multiple_of(j * r, r), r)
        return rc(x_ref.at[rows], raw_ref.at[y, rows], raw_s.at[i], raw_r.at[j, k], dev)

    def raw_block(j, b):
        return raw_ref.at[b, pl.ds(pl.multiple_of(j * r, r), r)]

    def raw_relay(j, b, off, dev, i):
        part = raw_ref.at[b, pl.ds(pl.multiple_of(j * r + off, half), half)]
        return rc(part, part, raw_s.at[i], raw_r.at[j, 2], dev)

    def raw_wait(j, b, k):
        rc(raw_block(j, b), raw_block(j, b), raw_s.at[0], raw_r.at[j, k], to_yp).wait_recv()

    gammas = [rc(g_ref, gv.at[y], g_s.at[i], g_r.at[k], dev) for i, (dev, k) in enumerate(((to_yp, 1), (to_ym, 0), (to_yo, 2)))]
    for cp in gammas:
        cp.start()
    raw_own(0, to_yp, 0, 1).start()
    raw_own(0, to_ym, 1, 0).start()
    raw_own(0, to_yo, 4, 2).start()

    def send_raw(j):
        raw_own(j, to_yp, 0, 1).start()
        raw_own(j, to_ym, 1, 0).start()
    loop(1, J, send_raw)

    def w1_copy(b, dev, i, k):
        return rc(w1_ref.at[:, pl.ds(pl.multiple_of(b * NS, 128), NS)], w1v.at[pl.ds(pl.multiple_of(y * KB, KB), KB)], w1_s.at[i], w1_r.at[k], dev)

    own_g = pltpu.make_async_copy(g_ref, gv.at[y], l_s.at[3])
    own_x = pltpu.make_async_copy(x_ref, xr, l_s.at[4])
    own_w1 = pltpu.make_async_copy(w1_ref.at[:, pl.ds(pl.multiple_of(y * NS, 128), NS)], w1v.at[pl.ds(pl.multiple_of(y * KB, KB), KB)], l_s.at[5])
    own_w2 = pltpu.make_async_copy(w2_ref, w2v, l_s.at[6])
    own_g.start()
    own_x.start()
    own_w1.start()
    own_w2.start()

    def xrow(j, b):
        return pl.multiple_of((j * 8 + b) * r, r)

    def x_own(j, dev, i, k):
        blk = xall_ref.at[pl.ds(xrow(j, x), r)]
        return rc(blk, blk, x_s.at[i], x_r.at[j, k], dev)

    def x_relay(j, b, off, dev, i):
        blk = xall_ref.at[pl.ds(pl.multiple_of(xrow(j, b) + off, half), half)]
        return rc(blk, blk, x_s.at[i], x_r.at[j, 2], dev)

    def x_wait(j, b, k):
        blk = xall_ref.at[pl.ds(xrow(j, b), r)]
        rc(blk, blk, x_s.at[0], x_r.at[j, k], to_xp).wait_recv()

    def d_copy(j, b, i):
        return rc(xall_ref.at[pl.ds(xrow(j, b), r)], xall_ref.at[pl.ds(xrow(j, 4 + b), r)], d_s.at[i], d_r.at[j, i], to_pt)

    def d_wait(j, b, i):
        blk = xall_ref.at[pl.ds(xrow(j, 4 + b), r)]
        rc(blk, blk, d_s.at[i], d_r.at[j, i], to_pt).wait_recv()

    def norm(j):
        raw_wait(j, yo, 2)
        loads = [pltpu.make_async_copy(raw_block(j, b), lr.at[i], l_s.at[i]) for i, b in enumerate((yp, ym, yo))]
        for cp in loads:
            cp.start()
        for cp in loads:
            cp.wait()
        rows = pl.ds(pl.multiple_of(j * r, r), r)
        parts = [(y, lambda: xr[rows]), (yp, lambda: lr[0]), (ym, lambda: lr[1]), (yo, lambda: lr[2])]
        total = jnp.zeros((r, 1), F32)
        for _, get in parts:
            total += jnp.sum(get().astype(F32), axis=1, keepdims=True)
        mean = total / K
        total = jnp.zeros((r, 1), F32)
        for _, get in parts:
            dev = get().astype(F32) - mean
            total += jnp.sum(dev * dev, axis=1, keepdims=True)
        inv = lax.rsqrt(total / K + LN_EPS)
        for b, get in parts:
            ln[:, pl.ds(pl.multiple_of(b * KB, KB), KB)] = ((get().astype(F32) - mean) * inv * gv[b]).astype(BF16)
        out = pltpu.make_async_copy(ln, xall_ref.at[pl.ds(xrow(j, x), r)], l_s.at[7])
        out.start()
        out.wait()
        x_own(j, to_xp, 0, 1).start()
        x_own(j, to_xm, 1, 0).start()
        d_copy(j, x, 0).start()

    def x_step(j):
        x_wait(j, xp, 0)
        x_wait(j, xm, 1)
        x_relay(j, xm, 0, to_xp, 2).start()
        x_relay(j, xp, half, to_xm, 3).start()
        d_copy(j, xp, 1).start()
        d_copy(j, xm, 2).start()

    def x_last(j):
        x_wait(j, xo, 2)
        d_copy(j, xo, 3).start()

    own_x.wait()
    own_g.wait()
    for b, k in ((yp, 0), (ym, 1), (yo, 2)):
        rc(gv.at[b], gv.at[b], g_s.at[0], g_r.at[k], to_yp).wait_recv()
    raw_wait(0, yp, 0)
    raw_wait(0, ym, 1)
    norm(0)

    def raw_step(j):
        raw_wait(j, yp, 0)
        raw_wait(j, ym, 1)
        raw_relay(j, ym, 0, to_yp, 2).start()
        raw_relay(j, yp, half, to_ym, 3).start()
    loop(1, J, raw_step)

    w1_sends = [w1_copy(b, dev, i, k) for i, (b, dev, k) in enumerate(((yp, to_yp, 1), (ym, to_ym, 0), (yo, to_yo, 2)))]
    for cp in w1_sends:
        cp.start()

    def norm_step(j):
        norm(j)

        @pl.when(j >= AHEAD)
        def _():
            x_step(j - AHEAD)

        @pl.when(j >= AHEAD + 2)
        def _():
            x_last(j - AHEAD - 2)
    loop(1, J, norm_step)

    def x_load(t):
        return pltpu.make_async_copy(xall_ref.at[pl.ds(pl.multiple_of(t * M, M), M)], xv.at[t % 2], xl_s.at[t % 2])

    def x_fetch(t):
        for i, b in enumerate((x, xp, xm, xo)):
            d_wait(t, b, i)
        x_load(t).start()

    x_fetch(0)
    own_w1.wait()
    own_w2.wait()
    for b, k in ((yp, 0), (ym, 1), (yo, 2)):
        blk = w1v.at[pl.ds(pl.multiple_of(b * KB, KB), KB)]
        rc(blk, blk, w1_s.at[0], w1_r.at[k], to_yp).wait_recv()

    def hcols(b):
        return pl.ds(pl.multiple_of(b * NS, 128), NS)

    def h_own(t, dev, i, k):
        blk = hv.at[t % HSLOTS, :, hcols(y)]
        return rc(blk, blk, h_s.at[t % HSLOTS, i], h_r.at[t, k], dev)

    def h_relay(t, b, off, dev, i):
        blk = hv.at[t % HSLOTS, pl.ds(off, M // 2), hcols(b)]
        return rc(blk, blk, q_s.at[t % HSLOTS, i], h_r.at[t, 2], dev)

    def h_wait(t, b, k):
        blk = hv.at[t % HSLOTS, :, hcols(b)]
        rc(blk, blk, h_s.at[0, 0], h_r.at[t, k], to_yp).wait_recv()

    def first(t):
        cut = NS * 4 // 7
        for lo, hi in ((0, cut), (cut, NS)):
            u = jnp.dot(xv[t % 2], w1v[:, lo:hi], preferred_element_type=F32)
            hv[t % HSLOTS, :, pl.ds(pl.multiple_of(y * NS + lo, 128), hi - lo)] = jax.nn.gelu(u, approximate=True).astype(BF16)

    def p_copy(j):
        return rc(pv.at[j % 2], pr.at[j % 2], p_s.at[j % 2], p_r.at[j], to_pt)

    def second(j):
        tn = DB // 2

        def cols(n):
            o = pl.ds(pl.multiple_of(n * tn, tn), tn)
            u = jnp.dot(hv[j % HSLOTS], w2v[:, o], preferred_element_type=F32)
            sv[j % 4, :, o] = u[:M // 2]
            pv[j % 2, :, o] = u[M // 2:]
        loop(0, 2, cols)

    def srow(b):
        return pl.multiple_of(b * r, r)

    def f_copy(j, off, dev, i, k):
        return rc(sv.at[j % 4, pl.ds(pl.multiple_of(srow(xo) + off, half), half)], hr.at[j % 2, k], f_s.at[j % 4, i], f_r.at[j, k], dev)

    def t_copy(j, b, dev, i, k):
        return rc(sv.at[j % 4, pl.ds(srow(b), r)], tr.at[j % 2, k], t_s.at[j % 4, i], t_r.at[j, k], dev)

    def add_partner(j):
        p_copy(j).wait_recv()
        sv[j % 4] += pr[j % 2]
        f_copy(j, 0, to_xp, 0, 1).start()
        f_copy(j, half, to_xm, 1, 0).start()

    def add_far(j):
        f_copy(j, 0, to_xp, 0, 1).wait_recv()
        f_copy(j, half, to_xm, 1, 0).wait_recv()
        sv[j % 4, pl.ds(srow(xp), half)] += hr[j % 2, 1]
        sv[j % 4, pl.ds(pl.multiple_of(srow(xm) + half, half), half)] += hr[j % 2, 0]
        t_copy(j, xp, to_xp, 0, 1).start()
        t_copy(j, xm, to_xm, 1, 0).start()

    def out_copy(j):
        rows = pl.ds(pl.multiple_of(j * r, r), r)
        return pltpu.make_async_copy(xr.at[rows], y_ref.at[rows], o_s)

    def finish(j):
        t_copy(j, xp, to_xp, 0, 1).wait_recv()
        t_copy(j, xm, to_xm, 1, 0).wait_recv()
        rows = pl.ds(pl.multiple_of(j * r, r), r)
        mlp = sv[j % 4, pl.ds(srow(x), r)] + tr[j % 2, 0] + tr[j % 2, 1]
        xr[rows] = (xr[rows].astype(F32) + mlp).astype(BF16)
        out_copy(j).start()

    def tick(t):
        def when(lag, f, hi=J):
            @pl.when(jnp.logical_and(t >= lag, t < hi + lag))
            def _():
                f(t - lag)

        def sent(j):
            h_own(j, to_yp, 0, 1).wait_send()
            h_own(j, to_ym, 1, 0).wait_send()
            h_relay(j, ym, 0, to_yp, 0).wait_send()
            h_relay(j, yp, M // 2, to_ym, 1).wait_send()
        when(3, sent)

        def start(j):
            x_load(j).wait()

            @pl.when(j + 1 < J)
            def _():
                x_fetch(j + 1)
            first(j)
            h_own(j, to_yp, 0, 1).start()
            h_own(j, to_ym, 1, 0).start()
        when(0, start)

        def relay(j):
            h_wait(j, yp, 0)
            h_wait(j, ym, 1)
            h_relay(j, ym, 0, to_yp, 0).start()
            h_relay(j, yp, M // 2, to_ym, 1).start()
        when(1, relay)
        when(5, finish)
        when(4, add_far)
        when(3, add_partner)

        def rest_step(j):
            x_step(j + J - AHEAD)
        when(2, rest_step, AHEAD)

        def rest_last(j):
            x_last(j + J - AHEAD - 2)
        when(2, rest_last, AHEAD + 2)

        def p_sent(j):
            p_copy(j).wait_send()
        when(4, p_sent)

        def out(j):
            h_wait(j, yo, 2)
            second(j)
            p_copy(j).start()
        when(2, out)

        def s_sent(j):
            f_copy(j, 0, to_xp, 0, 1).wait_send()
            f_copy(j, half, to_xm, 1, 0).wait_send()
            t_copy(j, xp, to_xp, 0, 1).wait_send()
            t_copy(j, xm, to_xm, 1, 0).wait_send()
        when(5, s_sent)
    loop(0, J + 5, tick)

    for cp in gammas + w1_sends:
        cp.wait_send()

    def drain(src, ss):
        rc(src, src, ss, raw_r.at[0, 0], to_yp).wait_send()
    drain(x_ref, raw_s.at[0])
    drain(x_ref, raw_s.at[1])
    rest = T // J * (J - 1) // 2
    drain(x_ref.at[pl.ds(0, rest)], raw_s.at[2])
    drain(x_ref.at[pl.ds(0, rest)], raw_s.at[3])
    drain(x_ref.at[pl.ds(0, r)], raw_s.at[4])
    for i in (0, 1):
        drain(xall_ref.at[pl.ds(0, T)], x_s.at[i])
    for i in (2, 3):
        drain(xall_ref.at[pl.ds(0, T // 2)], x_s.at[i])
    for i in range(4):
        drain(xall_ref.at[pl.ds(0, T)], d_s.at[i])
    pltpu.make_async_copy(xr, y_ref, o_s).wait()


def solution(mesh):
    assert mesh.shape["tp2"] == RING and mesh.shape["tp"] == 2 * RING
    row_spec = P(("data", "tp"), "tp2")

    def local_block(x_loc, scale_loc, w_in_loc, w_out_loc):
        T, KB = x_loc.shape
        NB, DB = w_out_loc.shape
        NS = NB // RING
        r = T // TICKS
        M = 8 * r
        K = RING * KB
        J = TICKS
        dma = pltpu.SemaphoreType.DMA
        any_spec = pl.BlockSpec(memory_space=pl.ANY)
        outs = pl.pallas_call(
            functools.partial(kernel, (T, KB, NS, DB, r, M)),
            out_shape=[
                jax.ShapeDtypeStruct((T, DB), BF16),
                jax.ShapeDtypeStruct((RING, T, KB), BF16),
                jax.ShapeDtypeStruct((J * M, K), BF16),
            ],
            in_specs=[any_spec] * 4,
            out_specs=[any_spec] * 3,
            scratch_shapes=[
                pltpu.VMEM((K, NS), BF16),
                pltpu.VMEM((NB, DB), BF16),
                pltpu.VMEM((2, M, K), BF16),
                pltpu.VMEM((HSLOTS, M, NB), BF16),
                pltpu.VMEM((4, M // 2, DB), F32),
                pltpu.VMEM((2, M // 2, DB), F32),
                pltpu.VMEM((2, M // 2, DB), F32),
                pltpu.VMEM((2, 2, r // 2, DB), F32),
                pltpu.VMEM((2, 2, r, DB), F32),
                pltpu.VMEM((T, DB), BF16),
                pltpu.VMEM((RING, 1, KB), F32),
                pltpu.VMEM((3, r, KB), BF16),
                pltpu.VMEM((r, K), BF16),
                dma((3,)), dma((3,)),
                dma((5,)), dma((J, 3)),
                dma((3,)), dma((3,)),
                dma((4,)), dma((J, 3)),
                dma((4,)), dma((J, 4)),
                dma((HSLOTS, 2)), dma((J, 3)), dma((HSLOTS, 2)),
                dma((2,)), dma((J,)),
                dma((4, 2)), dma((J, 2)),
                dma((4, 2)), dma((J, 2)),
                dma((8,)), dma((2,)), dma,
            ],
            compiler_params=pltpu.CompilerParams(collective_id=0, has_side_effects=True, vmem_limit_bytes=67043328),
        )(x_loc, scale_loc.reshape(1, KB), w_in_loc, w_out_loc)
        return outs[0]

    return jax.shard_map(local_block, mesh=mesh, in_specs=(row_spec, P("tp2"), P("tp2", "tp"), P("tp", "tp2")), out_specs=row_spec, check_vma=False)
```

```python
import functools

import jax
import jax.numpy as jnp
from jax import lax
from jax.experimental import pallas as pl
from jax.experimental.pallas import tpu as pltpu
from jax.sharding import PartitionSpec as P

LN_EPS = 1e-6
RING = 4
CHUNKS = 16
FULL = 14
SPLIT = 2
TICKS = FULL + (CHUNKS - FULL) * SPLIT
AHEAD = 4
CATCH = 8
RSLOTS, HSLOTS, SSLOTS, VSLOTS, FSLOTS = 8, 5, 4, 3, 4
MESH = pl.DeviceIdType.MESH
BF16, F32 = jnp.bfloat16, jnp.float32


def kernel(dims, x_ref, g_ref, w1_ref, w2_ref, y_ref, raw_ref, xall_ref, w1v, w2v, xv, hv, sv, pv, pr, hr, tr, xr, gv, lr, ln,
           g_s, g_r, raw_s, raw_r, w1_s, w1_r, x_s, x_r, d_s, d_r, h_s, h_r, q_s, p_s, p_r, f_s, f_r, t_s, t_r, l_s, xl_s, o_s):
    T, KB, NS, DB, r = dims
    J, K, small = CHUNKS, RING * KB, r // SPLIT
    half = r // 2
    d = lax.axis_index("data")
    y = lax.axis_index("tp2")
    tp = lax.axis_index("tp")
    x, c = tp // 2, tp % 2
    yp, yo, ym = (y + 1) % RING, (y + 2) % RING, (y + 3) % RING
    xp, xo, xm = (x + 1) % RING, (x + 2) % RING, (x + 3) % RING
    to_yp, to_ym, to_yo = (d, yp, tp), (d, ym, tp), (d, yo, tp)
    to_xp, to_xm = (d, y, xp * 2 + c), (d, y, xm * 2 + c)
    to_pt = (d, y, x * 2 + 1 - c)

    def rc(src, dst, ss, rs, dev):
        return pltpu.make_async_remote_copy(src_ref=src, dst_ref=dst, send_sem=ss, recv_sem=rs, device_id=dev, device_id_type=MESH)

    def arrived(ref, sem):
        rc(ref, ref, o_s, sem, to_pt).wait_recv()

    def left(ref, sem):
        rc(ref, ref, sem, o_s, to_pt).wait_send()

    def loop(lo, hi, f):
        def body(i, carry):
            f(i)
            return carry
        lax.fori_loop(lo, hi, body, 0)

    barrier = pltpu.get_barrier_semaphore()
    for dev in (to_yp, to_ym, to_yo, to_xp, to_xm, to_pt):
        pl.semaphore_signal(barrier, inc=1, device_id=dev, device_id_type=MESH)
    pl.semaphore_wait(barrier, 6)

    def raw_block(j, b):
        return raw_ref.at[b, pl.ds(pl.multiple_of(j * r, r), r)]

    def raw_own(j, dev, i, k=0):
        rows = pl.ds(pl.multiple_of(j * r, r), r)
        return rc(x_ref.at[rows], raw_ref.at[y, rows], raw_s.at[i], raw_r.at[j % RSLOTS, k], dev)

    def raw_relay(j, b, off, dev, i):
        part = raw_ref.at[b, pl.ds(pl.multiple_of(j * r + off, half), half)]
        return rc(part, part, raw_s.at[i], raw_r.at[j % RSLOTS, 1], dev)

    def send_raw(j):
        raw_own(j, to_yp, 0).start()
        raw_own(j, to_ym, 1).start()

    send_raw(0)
    raw_own(0, to_yo, 4, 1).start()
    gammas = [rc(g_ref, gv.at[y], g_s, g_r, dev) for dev in (to_yp, to_ym, to_yo)]
    for cp in gammas:
        cp.start()
    for j in range(1, AHEAD):
        send_raw(j)

    cut = NS * 4 // 7
    parts = ((0, cut), (cut, NS))

    def w1_block(b, part):
        lo, hi = parts[part]
        return w1v.at[pl.ds(pl.multiple_of(b * KB, KB), KB), pl.ds(lo, hi - lo)]

    def w1_copy(b, dev, part):
        lo, hi = parts[part]
        cols = w1_ref.at[:, pl.ds(pl.multiple_of(b * NS + lo, 128), hi - lo)]
        return rc(cols, w1_block(y, part), w1_s.at[part], w1_r.at[part], dev)

    def w1_wait(part):
        lo, hi = parts[part]
        arrived(w1v.at[pl.ds(0, 3 * KB), pl.ds(lo, hi - lo)], w1_r.at[part])

    own_g = pltpu.make_async_copy(g_ref, gv.at[y], l_s.at[3])
    own_x = pltpu.make_async_copy(x_ref, xr, l_s.at[4])
    own_w1 = pltpu.make_async_copy(w1_ref.at[:, pl.ds(pl.multiple_of(y * NS, 128), NS)], w1v.at[pl.ds(pl.multiple_of(y * KB, KB), KB)], l_s.at[5])
    own_w2 = pltpu.make_async_copy(w2_ref, w2v, l_s.at[6])
    own_g.start()
    own_x.start()
    own_w1.start()
    own_w2.start()

    def x_own(j, dev, i):
        return rc(xall_ref.at[j, x], xall_ref.at[j, x], x_s.at[i], x_r.at[j, 0], dev)

    def x_relay(j, b, off, dev, i):
        blk = xall_ref.at[j, b, pl.ds(off, half)]
        return rc(blk, blk, x_s.at[i], x_r.at[j, 1], dev)

    def d_copy(j, b, i):
        return rc(xall_ref.at[j, b], xall_ref.at[j, 4 + b], d_s.at[i], d_r.at[j], to_pt)

    def norm(j):
        arrived(raw_block(j, yo), raw_r.at[j % RSLOTS, 1])
        loads = [pltpu.make_async_copy(raw_block(j, b), lr.at[i], l_s.at[i]) for i, b in enumerate((yp, ym, yo))]
        for cp in loads:
            cp.start()
        for cp in loads:
            cp.wait()
        rows = pl.ds(pl.multiple_of(j * r, r), r)
        blocks = [(y, lambda: xr[rows]), (yp, lambda: lr[0]), (ym, lambda: lr[1]), (yo, lambda: lr[2])]
        total = jnp.zeros((r, 1), F32)
        for _, get in blocks:
            total += jnp.sum(get().astype(F32), axis=1, keepdims=True)
        mean = total / K
        total = jnp.zeros((r, 1), F32)
        for _, get in blocks:
            dev = get().astype(F32) - mean
            total += jnp.sum(dev * dev, axis=1, keepdims=True)
        inv = lax.rsqrt(total / K + LN_EPS)
        for b, get in blocks:
            ln[:, pl.ds(pl.multiple_of(b * KB, KB), KB)] = ((get().astype(F32) - mean) * inv * gv[b]).astype(BF16)
        out = pltpu.make_async_copy(ln, xall_ref.at[j, x], l_s.at[7])
        out.start()
        out.wait()
        x_own(j, to_xp, 0).start()
        x_own(j, to_xm, 1).start()
        d_copy(j, x, 0).start()

    def x_step(j):
        arrived(xall_ref.at[j, pl.ds(0, 2)], x_r.at[j, 0])
        x_relay(j, xm, 0, to_xp, 2).start()
        x_relay(j, xp, half, to_xm, 3).start()
        d_copy(j, xp, 1).start()
        d_copy(j, xm, 2).start()

    def x_last(j):
        arrived(xall_ref.at[j, xo], x_r.at[j, 1])
        d_copy(j, xo, 3).start()

    def raw_wait(j):
        arrived(raw_ref.at[pl.ds(0, 2), pl.ds(0, r)], raw_r.at[j % RSLOTS, 0])

    def raw_step(j):
        raw_wait(j)
        raw_relay(j, ym, 0, to_yp, 2).start()
        raw_relay(j, yp, half, to_ym, 3).start()

    def raw_tick(j):
        raw_step(j)

        send_raw(j + AHEAD)

        @pl.when(jnp.logical_and(j >= 3, j < J - AHEAD))
        def _():
            norm(j - 2)

    own_x.wait()
    own_g.wait()
    raw_wait(0)
    send_raw(AHEAD)
    arrived(gv.at[pl.ds(0, 3)], g_r)
    norm(0)
    loop(1, J - AHEAD, raw_tick)
    loop(J - AHEAD, J, raw_step)
    w1_sends = [w1_copy(b, dev, part) for part in (0, 1) for b, dev in ((yp, to_yp), (ym, to_ym), (yo, to_yo))]
    for cp in w1_sends:
        cp.start()
    loop(J - AHEAD - 2, J, norm)
    loop(0, J, x_step)
    loop(0, 3, x_last)

    def full(t):
        return (t, t, 0, r)

    def short(t):
        return (t, FULL + (t - FULL) // SPLIT, (t - FULL) % SPLIT * small, small)

    def x_load(k):
        t, j, off, n = k
        rows = pl.ds(0, n) if n == r else pl.ds(pl.multiple_of(off, small), n)
        return pltpu.make_async_copy(xall_ref.at[j, :, rows], xv.at[t % 2, :, pl.ds(0, n)], xl_s.at[t % 2])

    def x_fetch(k):
        arrived_rows = xall_ref.at[k[1], pl.ds(4, 4)]
        if k[3] == r:
            arrived(arrived_rows, d_r.at[k[1]])
        else:
            @pl.when(k[2] == 0)
            def _():
                arrived(arrived_rows, d_r.at[k[1]])
        x_load(k).start()

    x_fetch(full(0))
    own_w1.wait()
    own_w2.wait()
    w1_wait(0)

    def hcols(b, lo=0, hi=NS):
        return pl.ds(pl.multiple_of(b * NS + lo, 128), hi - lo)

    def h_own(k, dev, part):
        t, n = k[0], 8 * k[3]
        lo, hi = parts[part]
        blk = hv.at[t % HSLOTS, pl.ds(0, n), hcols(y, lo, hi)]
        return rc(blk, blk, h_s.at[t % HSLOTS], h_r.at[t % HSLOTS, 0], dev)

    def h_relay(k, b, side, dev):
        t, n = k[0], 4 * k[3]
        blk = hv.at[t % HSLOTS, pl.ds(side * n, n), hcols(b)]
        return rc(blk, blk, q_s.at[t % HSLOTS], h_r.at[t % HSLOTS, 1], dev)

    def h_bytes(k, blocks):
        return hv.at[k[0] % HSLOTS, pl.ds(0, 8 * k[3]), pl.ds(0, blocks * NS)]

    def sent(k):
        left(h_bytes(k, 2), h_s.at[k[0] % HSLOTS])
        left(h_bytes(k, 1), q_s.at[k[0] % HSLOTS])

    def start(k, fetch, first):
        t, n = k[0], k[3]
        x_load(k).wait()
        fetch()
        for part, (lo, hi) in enumerate(parts):
            if part == 1 and first is not None:
                @pl.when(first)
                def _():
                    w1_wait(1)
            rows = xv[t % 2, :, :n].reshape(8 * n, K)
            u = jnp.dot(rows, w1v[:, lo:hi], preferred_element_type=F32)
            hv[t % HSLOTS, :8 * n, hcols(y, lo, hi)] = jax.nn.gelu(u, approximate=True).astype(BF16)
            h_own(k, to_yp, part).start()
            h_own(k, to_ym, part).start()

    def relay(k):
        arrived(h_bytes(k, 2), h_r.at[k[0] % HSLOTS, 0])
        h_relay(k, ym, 0, to_yp).start()
        h_relay(k, yp, 1, to_ym).start()

    def p_copy(k):
        t, n = k[0], 4 * k[3]
        return rc(pv.at[t % 2, pl.ds(0, n)], pr.at[t % VSLOTS, pl.ds(0, n)], p_s.at[t % 2], p_r.at[t % VSLOTS], to_pt)

    def p_sent(k):
        p_copy(k).wait_send()

    def second(k):
        t, n = k[0], 4 * k[3]
        arrived(h_bytes(k, 1), h_r.at[t % HSLOTS, 1])
        tn = DB // 2

        def cols(i):
            o = pl.ds(pl.multiple_of(i * tn, tn), tn)
            u = jnp.dot(hv[t % HSLOTS, :2 * n], w2v[:, o], preferred_element_type=F32)
            sv[t % SSLOTS, :n, o] = u[:n]
            pv[t % 2, :n, o] = u[n:]
        loop(0, 2, cols)
        p_copy(k).start()

    def s_rows(k, b):
        return pl.ds(pl.multiple_of(b * k[3], k[3]), k[3])

    def f_copy(k, side, dev):
        t, n = k[0], k[3]
        cols = pl.ds(side * (DB // 2), DB // 2)
        return rc(sv.at[t % SSLOTS, s_rows(k, xo), cols], hr.at[t % FSLOTS, side, pl.ds(0, n)], f_s.at[t % SSLOTS], f_r.at[t % FSLOTS], dev)

    def t_copy(k, b, dev, q):
        t, n = k[0], k[3]
        return rc(sv.at[t % SSLOTS, s_rows(k, b)], tr.at[t % VSLOTS, q, pl.ds(0, n)], t_s.at[t % SSLOTS], t_r.at[t % VSLOTS], dev)

    def add_partner(k):
        t, n = k[0], 4 * k[3]
        p_copy(k).wait_recv()
        sv[t % SSLOTS, :n] += pr[t % VSLOTS, :n]
        f_copy(k, 0, to_xp).start()
        f_copy(k, 1, to_xm).start()

    def add_far(k):
        t, n = k[0], k[3]
        m = DB // 2
        arrived(hr.at[t % FSLOTS, :, pl.ds(0, n)], f_r.at[t % FSLOTS])
        sv[t % SSLOTS, s_rows(k, xp), :m] += hr[t % FSLOTS, 0, :n]
        sv[t % SSLOTS, s_rows(k, xm), m:] += hr[t % FSLOTS, 1, :n]
        t_copy(k, xp, to_xp, 1).start()
        t_copy(k, xm, to_xm, 0).start()

    def finish(k):
        t, j, off, n = k
        arrived(tr.at[t % VSLOTS, :, pl.ds(0, n)], t_r.at[t % VSLOTS])
        rows = pl.ds(pl.multiple_of(j * r + off, n), n)
        mlp = sv[t % SSLOTS, s_rows(k, x)] + tr[t % VSLOTS, 0, :n] + tr[t % VSLOTS, 1, :n]
        xr[rows] = (xr[rows].astype(F32) + mlp).astype(BF16)
        pltpu.make_async_copy(xr.at[rows], y_ref.at[rows], o_s).start()

    def s_sent(k):
        t, n = k[0], k[3]
        left(sv.at[t % SSLOTS, pl.ds(0, n)], f_s.at[t % SSLOTS])
        left(sv.at[t % SSLOTS, pl.ds(0, 2 * n)], t_s.at[t % SSLOTS])

    def tick(t):
        def when(lag, f, since=0):
            @pl.when(jnp.logical_and(t >= max(lag, since), t < FULL + lag))
            def _():
                f(full(t - lag))

            @pl.when(t >= FULL + lag)
            def _():
                f(short(t - lag))

        def begin(k):
            def fetch():
                if k[3] == r:
                    @pl.when(t + 1 < FULL)
                    def _():
                        x_fetch(full(t + 1))

                    @pl.when(t + 1 == FULL)
                    def _():
                        x_fetch(short(t + 1))
                else:
                    @pl.when(t + 1 < TICKS)
                    def _():
                        x_fetch(short(t + 1))
            start(k, fetch, t == 0 if k[3] == r else None)
        when(3, sent)
        when(0, begin)
        when(1, relay)
        when(3, add_partner)

        @pl.when(t + 3 < J)
        def _():
            x_last(t + 3)
        when(4, p_sent)
        when(2, second)

        @pl.when(jnp.logical_and(t >= 4, t <= CATCH))
        def _():
            add_far(full(t - 4))
        when(3, add_far, CATCH)

        @pl.when(jnp.logical_and(t >= 5, t <= CATCH + 1))
        def _():
            finish(full(t - 5))
        when(4, finish, CATCH + 1)
        when(5, s_sent)
    loop(0, TICKS, tick)

    n4, n3, n2, n1 = (short(TICKS - i) for i in (4, 3, 2, 1))
    n5 = full(TICKS - 5)
    relay(n1)
    add_partner(n3)
    p_sent(n4)
    second(n2)
    add_far(n3)
    p_sent(n3)
    s_sent(n5)
    second(n1)
    add_partner(n2)
    finish(n4)
    add_partner(n1)
    add_far(n2)
    finish(n3)
    add_far(n1)
    finish(n2)
    finish(n1)
    for k in (n3, n2, n1):
        sent(k)
    p_sent(n2)
    p_sent(n1)
    for k in (n4, n3, n2, n1):
        s_sent(k)

    left(gv.at[pl.ds(0, 3)], g_s)
    for part, (lo, hi) in enumerate(parts):
        left(w1v.at[pl.ds(0, 3 * KB), pl.ds(lo, hi - lo)], w1_s.at[part])
    left(x_ref, raw_s.at[0])
    left(x_ref, raw_s.at[1])
    rest = pl.ds(0, (J - 1) * half)
    left(x_ref.at[rest], raw_s.at[2])
    left(x_ref.at[rest], raw_s.at[3])
    left(x_ref.at[pl.ds(0, r)], raw_s.at[4])
    for i in (0, 1):
        left(xall_ref.at[pl.ds(0, J // 8)], x_s.at[i])
    for i in (2, 3):
        left(xall_ref.at[pl.ds(0, J // 16)], x_s.at[i])
    for i in range(4):
        left(xall_ref.at[pl.ds(0, J // 8)], d_s.at[i])
    pltpu.make_async_copy(xr, y_ref, o_s).wait()


def solution(mesh):
    assert mesh.shape["tp2"] == RING and mesh.shape["tp"] == 2 * RING
    row_spec = P(("data", "tp"), "tp2")

    def local_block(x_loc, scale_loc, w_in_loc, w_out_loc):
        T, KB = x_loc.shape
        NB, DB = w_out_loc.shape
        NS, K, r = NB // RING, RING * KB, T // CHUNKS
        dma = pltpu.SemaphoreType.DMA
        any_spec = pl.BlockSpec(memory_space=pl.ANY)
        outs = pl.pallas_call(
            functools.partial(kernel, (T, KB, NS, DB, r)),
            out_shape=[
                jax.ShapeDtypeStruct((T, DB), BF16),
                jax.ShapeDtypeStruct((RING, T, KB), BF16),
                jax.ShapeDtypeStruct((CHUNKS, 8, r, K), BF16),
            ],
            in_specs=[any_spec] * 4,
            out_specs=[any_spec] * 3,
            scratch_shapes=[
                pltpu.VMEM((K, NS), BF16),
                pltpu.VMEM((NB, DB), BF16),
                pltpu.VMEM((2, 8, r, K), BF16),
                pltpu.VMEM((HSLOTS, 8 * r, NB), BF16),
                pltpu.VMEM((SSLOTS, 4 * r, DB), F32),
                pltpu.VMEM((2, 4 * r, DB), F32),
                pltpu.VMEM((VSLOTS, 4 * r, DB), F32),
                pltpu.VMEM((FSLOTS, 2, r, DB // 2), F32),
                pltpu.VMEM((VSLOTS, 2, r, DB), F32),
                pltpu.VMEM((T, DB), BF16),
                pltpu.VMEM((RING, 1, KB), F32),
                pltpu.VMEM((3, r, KB), BF16),
                pltpu.VMEM((r, K), BF16),
                dma, dma,
                dma((5,)), dma((RSLOTS, 2)),
                dma((2,)), dma((2,)),
                dma((4,)), dma((CHUNKS, 2)),
                dma((4,)), dma((CHUNKS,)),
                dma((HSLOTS,)), dma((HSLOTS, 2)), dma((HSLOTS,)),
                dma((2,)), dma((VSLOTS,)),
                dma((SSLOTS,)), dma((FSLOTS,)),
                dma((SSLOTS,)), dma((VSLOTS,)),
                dma((8,)), dma((2,)), dma,
            ],
            compiler_params=pltpu.CompilerParams(collective_id=0, has_side_effects=True, vmem_limit_bytes=67043328),
        )(x_loc, scale_loc.reshape(1, KB), w_in_loc, w_out_loc)
        return outs[0]

    return jax.shard_map(local_block, mesh=mesh, in_specs=(row_spec, P("tp2"), P("tp2", "tp"), P("tp", "tp2")), out_specs=row_spec, check_vma=False)
```

```python
import functools

import jax
import jax.numpy as jnp
from jax import lax
from jax.experimental import pallas as pl
from jax.experimental.pallas import tpu as pltpu
from jax.sharding import PartitionSpec as P

LN_EPS = 1e-6
RING = 4
CHUNKS = 16
FULL = 12
SPLIT = 2
TICKS = FULL + (CHUNKS - FULL) * SPLIT
AHEAD = 4
CATCH = 8
RSLOTS, HSLOTS, SSLOTS, VSLOTS, FSLOTS = 8, 5, 4, 3, 4
MESH = pl.DeviceIdType.MESH
BF16, F32 = jnp.bfloat16, jnp.float32


def kernel(dims, x_ref, g_ref, w1_ref, w2_ref, xr, raw_ref, xall_ref, w1v, w2v, xv, hv, sv, pv, pr, hr, tr, gv, lr, ln,
           g_s, g_r, raw_s, raw_r, w1_s, w1_r, x_s, x_r, d_s, d_r, h_s, h_r, q_s, p_s, p_r, f_s, f_r, t_s, t_r, l_s, xl_s, o_s):
    T, KB, NS, DB, r = dims
    J, K, small = CHUNKS, RING * KB, r // SPLIT
    half = r // 2
    d = lax.axis_index("data")
    y = lax.axis_index("tp2")
    tp = lax.axis_index("tp")
    x, c = tp // 2, tp % 2
    yp, yo, ym = (y + 1) % RING, (y + 2) % RING, (y + 3) % RING
    xp, xo, xm = (x + 1) % RING, (x + 2) % RING, (x + 3) % RING
    to_yp, to_ym, to_yo = (d, yp, tp), (d, ym, tp), (d, yo, tp)
    to_xp, to_xm = (d, y, xp * 2 + c), (d, y, xm * 2 + c)
    to_pt = (d, y, x * 2 + 1 - c)

    def rc(src, dst, ss, rs, dev):
        return pltpu.make_async_remote_copy(src_ref=src, dst_ref=dst, send_sem=ss, recv_sem=rs, device_id=dev, device_id_type=MESH)

    def arrived(ref, sem):
        rc(ref, ref, o_s, sem, to_pt).wait_recv()

    def left(ref, sem):
        rc(ref, ref, sem, o_s, to_pt).wait_send()

    def loop(lo, hi, f):
        def body(i, carry):
            f(i)
            return carry
        lax.fori_loop(lo, hi, body, 0)

    barrier = pltpu.get_barrier_semaphore()
    for dev in (to_yp, to_ym, to_yo, to_xp, to_xm, to_pt):
        pl.semaphore_signal(barrier, inc=1, device_id=dev, device_id_type=MESH)
    pl.semaphore_wait(barrier, 6)

    def raw_block(j, b):
        return raw_ref.at[b, pl.ds(pl.multiple_of(j * r, r), r)]

    def raw_own(j, dev, i, k=0):
        rows = pl.ds(pl.multiple_of(j * r, r), r)
        return rc(x_ref.at[rows], raw_ref.at[y, rows], raw_s.at[i], raw_r.at[j % RSLOTS, k], dev)

    def raw_relay(j, b, off, dev, i):
        part = raw_ref.at[b, pl.ds(pl.multiple_of(j * r + off, half), half)]
        return rc(part, part, raw_s.at[i], raw_r.at[j % RSLOTS, 1], dev)

    def send_raw(j):
        raw_own(j, to_yp, 0).start()
        raw_own(j, to_ym, 1).start()

    send_raw(0)
    raw_own(0, to_yo, 4, 1).start()
    gammas = [rc(g_ref, gv.at[y], g_s, g_r, dev) for dev in (to_yp, to_ym, to_yo)]
    for cp in gammas:
        cp.start()
    for j in range(1, AHEAD):
        send_raw(j)

    cut = NS * 4 // 7
    parts = ((0, cut), (cut, NS))

    def w1_block(b, part):
        lo, hi = parts[part]
        return w1v.at[pl.ds(pl.multiple_of(b * KB, KB), KB), pl.ds(lo, hi - lo)]

    def w1_copy(b, dev, part):
        lo, hi = parts[part]
        cols = w1_ref.at[:, pl.ds(pl.multiple_of(b * NS + lo, 128), hi - lo)]
        return rc(cols, w1_block(y, part), w1_s.at[part], w1_r.at[part], dev)

    def w1_wait(part):
        lo, hi = parts[part]
        arrived(w1v.at[pl.ds(0, 3 * KB), pl.ds(lo, hi - lo)], w1_r.at[part])

    own_g = pltpu.make_async_copy(g_ref, gv.at[y], l_s.at[3])
    own_x = pltpu.make_async_copy(x_ref, xr, l_s.at[4])
    own_w1 = pltpu.make_async_copy(w1_ref.at[:, pl.ds(pl.multiple_of(y * NS, 128), NS)], w1v.at[pl.ds(pl.multiple_of(y * KB, KB), KB)], l_s.at[5])
    own_w2 = pltpu.make_async_copy(w2_ref, w2v, l_s.at[6])
    own_g.start()
    own_x.start()
    own_w1.start()
    own_w2.start()

    def x_own(j, dev, i):
        return rc(xall_ref.at[j, x], xall_ref.at[j, x], x_s.at[i], x_r.at[j, 0], dev)

    def x_relay(j, b, off, dev, i):
        blk = xall_ref.at[j, b, pl.ds(off, half)]
        return rc(blk, blk, x_s.at[i], x_r.at[j, 1], dev)

    def d_copy(j, b, i):
        return rc(xall_ref.at[j, b], xall_ref.at[j, 4 + b], d_s.at[i], d_r.at[j], to_pt)

    def norm(j):
        arrived(raw_block(j, yo), raw_r.at[j % RSLOTS, 1])
        loads = [pltpu.make_async_copy(raw_block(j, b), lr.at[i], l_s.at[i]) for i, b in enumerate((yp, ym, yo))]
        for cp in loads:
            cp.start()
        for cp in loads:
            cp.wait()
        rows = pl.ds(pl.multiple_of(j * r, r), r)
        blocks = [(y, lambda: xr[rows]), (yp, lambda: lr[0]), (ym, lambda: lr[1]), (yo, lambda: lr[2])]
        total = jnp.zeros((r, 1), F32)
        for _, get in blocks:
            total += jnp.sum(get().astype(F32), axis=1, keepdims=True)
        mean = total / K
        total = jnp.zeros((r, 1), F32)
        for _, get in blocks:
            dev = get().astype(F32) - mean
            total += jnp.sum(dev * dev, axis=1, keepdims=True)
        inv = lax.rsqrt(total / K + LN_EPS)
        for b, get in blocks:
            ln[:, pl.ds(pl.multiple_of(b * KB, KB), KB)] = ((get().astype(F32) - mean) * inv * gv[b]).astype(BF16)
        out = pltpu.make_async_copy(ln, xall_ref.at[j, x], l_s.at[7])
        out.start()
        out.wait()
        x_own(j, to_xp, 0).start()
        x_own(j, to_xm, 1).start()
        d_copy(j, x, 0).start()

    def x_step(j):
        arrived(xall_ref.at[j, pl.ds(0, 2)], x_r.at[j, 0])
        x_relay(j, xm, 0, to_xp, 2).start()
        x_relay(j, xp, half, to_xm, 3).start()
        d_copy(j, xp, 1).start()
        d_copy(j, xm, 2).start()

    def x_last(j):
        arrived(xall_ref.at[j, xo], x_r.at[j, 1])
        d_copy(j, xo, 3).start()

    def raw_wait(j):
        arrived(raw_ref.at[pl.ds(0, 2), pl.ds(0, r)], raw_r.at[j % RSLOTS, 0])

    def raw_step(j):
        raw_wait(j)
        raw_relay(j, ym, 0, to_yp, 2).start()
        raw_relay(j, yp, half, to_ym, 3).start()

    def raw_tick(j):
        raw_step(j)

        send_raw(j + AHEAD)

        @pl.when(jnp.logical_and(j >= 3, j < J - AHEAD))
        def _():
            norm(j - 2)

    own_x.wait()
    own_g.wait()
    raw_wait(0)
    send_raw(AHEAD)
    arrived(gv.at[pl.ds(0, 3)], g_r)
    norm(0)
    loop(1, J - AHEAD, raw_tick)
    loop(J - AHEAD, J, raw_step)
    w1_sends = [w1_copy(b, dev, part) for part in (0, 1) for b, dev in ((yp, to_yp), (ym, to_ym), (yo, to_yo))]
    for cp in w1_sends:
        cp.start()
    loop(J - AHEAD - 2, J, norm)
    loop(0, J, x_step)
    loop(0, 3, x_last)

    def full(t):
        return (t, t, 0, r)

    def short(t):
        return (t, FULL + (t - FULL) // SPLIT, (t - FULL) % SPLIT * small, small)

    def x_load(k):
        t, j, off, n = k
        rows = pl.ds(0, n) if n == r else pl.ds(pl.multiple_of(off, small), n)
        return pltpu.make_async_copy(xall_ref.at[j, :, rows], xv.at[t % 2, :, pl.ds(0, n)], xl_s.at[t % 2])

    def x_fetch(k):
        arrived_rows = xall_ref.at[k[1], pl.ds(4, 4)]
        if k[3] == r:
            arrived(arrived_rows, d_r.at[k[1]])
        else:
            @pl.when(k[2] == 0)
            def _():
                arrived(arrived_rows, d_r.at[k[1]])
        x_load(k).start()

    x_fetch(full(0))
    own_w1.wait()
    own_w2.wait()
    w1_wait(0)

    def hcols(b, lo=0, hi=NS):
        return pl.ds(pl.multiple_of(b * NS + lo, 128), hi - lo)

    def h_own(k, dev, part):
        t, n = k[0], 8 * k[3]
        lo, hi = parts[part]
        blk = hv.at[t % HSLOTS, pl.ds(0, n), hcols(y, lo, hi)]
        return rc(blk, blk, h_s.at[t % HSLOTS], h_r.at[t % HSLOTS, 0], dev)

    def h_relay(k, b, side, dev):
        t, n = k[0], 4 * k[3]
        blk = hv.at[t % HSLOTS, pl.ds(side * n, n), hcols(b)]
        return rc(blk, blk, q_s.at[t % HSLOTS], h_r.at[t % HSLOTS, 1], dev)

    def h_bytes(k, blocks):
        return hv.at[k[0] % HSLOTS, pl.ds(0, 8 * k[3]), pl.ds(0, blocks * NS)]

    def sent(k):
        left(h_bytes(k, 2), h_s.at[k[0] % HSLOTS])
        left(h_bytes(k, 1), q_s.at[k[0] % HSLOTS])

    def start(k, fetch, first):
        t, n = k[0], k[3]
        x_load(k).wait()
        fetch()
        for part, (lo, hi) in enumerate(parts):
            if part == 1 and first is not None:
                @pl.when(first)
                def _():
                    w1_wait(1)
            rows = xv[t % 2, :, :n].reshape(8 * n, K)
            u = jnp.dot(rows, w1v[:, lo:hi], preferred_element_type=F32)
            hv[t % HSLOTS, :8 * n, hcols(y, lo, hi)] = jax.nn.gelu(u, approximate=True).astype(BF16)
            h_own(k, to_yp, part).start()
            h_own(k, to_ym, part).start()

    def relay(k):
        arrived(h_bytes(k, 2), h_r.at[k[0] % HSLOTS, 0])
        h_relay(k, ym, 0, to_yp).start()
        h_relay(k, yp, 1, to_ym).start()

    def p_copy(k):
        t, n = k[0], 4 * k[3]
        return rc(pv.at[t % 2, pl.ds(0, n)], pr.at[t % VSLOTS, pl.ds(0, n)], p_s.at[t % 2], p_r.at[t % VSLOTS], to_pt)

    def p_sent(k):
        p_copy(k).wait_send()

    def second(k):
        t, n = k[0], 4 * k[3]
        arrived(h_bytes(k, 1), h_r.at[t % HSLOTS, 1])
        tn = DB // 2

        def cols(i):
            o = pl.ds(pl.multiple_of(i * tn, tn), tn)
            u = jnp.dot(hv[t % HSLOTS, :2 * n], w2v[:, o], preferred_element_type=F32)
            sv[t % SSLOTS, :n, o] = u[:n]
            pv[t % 2, :n, o] = u[n:]
        loop(0, 2, cols)
        p_copy(k).start()

    def second_part(k, blocks, add):
        t, n = k[0], 4 * k[3]
        tn = DB // 2

        def cols(i):
            o = pl.ds(pl.multiple_of(i * tn, tn), tn)
            u = sum(jnp.dot(hv[t % HSLOTS, :2 * n, hcols(b)], w2v[pl.ds(pl.multiple_of(b * NS, NS), NS), o], preferred_element_type=F32) for b in blocks)
            if add:
                sv[t % SSLOTS, :n, o] += u[:n]
                pv[t % 2, :n, o] += u[n:]
            else:
                sv[t % SSLOTS, :n, o] = u[:n]
                pv[t % 2, :n, o] = u[n:]
        loop(0, 2, cols)

    def second_early(k):
        second_part(k, (y, yp, ym), False)

    def second_late(k):
        arrived(h_bytes(k, 1), h_r.at[k[0] % HSLOTS, 1])
        second_part(k, (yo,), True)
        p_copy(k).start()

    def s_rows(k, b):
        return pl.ds(pl.multiple_of(b * k[3], k[3]), k[3])

    def f_copy(k, side, dev):
        t, n = k[0], k[3]
        cols = pl.ds(side * (DB // 2), DB // 2)
        return rc(sv.at[t % SSLOTS, s_rows(k, xo), cols], hr.at[t % FSLOTS, side, pl.ds(0, n)], f_s.at[t % SSLOTS], f_r.at[t % FSLOTS], dev)

    def t_copy(k, b, dev, q):
        t, n = k[0], k[3]
        return rc(sv.at[t % SSLOTS, s_rows(k, b)], tr.at[t % VSLOTS, q, pl.ds(0, n)], t_s.at[t % SSLOTS], t_r.at[t % VSLOTS], dev)

    def add_partner(k):
        t, n = k[0], 4 * k[3]
        p_copy(k).wait_recv()
        sv[t % SSLOTS, :n] += pr[t % VSLOTS, :n]
        f_copy(k, 0, to_xp).start()
        f_copy(k, 1, to_xm).start()

    def add_far(k):
        t, n = k[0], k[3]
        m = DB // 2
        arrived(hr.at[t % FSLOTS, :, pl.ds(0, n)], f_r.at[t % FSLOTS])
        sv[t % SSLOTS, s_rows(k, xp), :m] += hr[t % FSLOTS, 0, :n]
        sv[t % SSLOTS, s_rows(k, xm), m:] += hr[t % FSLOTS, 1, :n]
        t_copy(k, xp, to_xp, 1).start()
        t_copy(k, xm, to_xm, 0).start()

    def finish(k):
        t, j, off, n = k
        arrived(tr.at[t % VSLOTS, :, pl.ds(0, n)], t_r.at[t % VSLOTS])
        rows = pl.ds(pl.multiple_of(j * r + off, n), n)
        mlp = sv[t % SSLOTS, s_rows(k, x)] + tr[t % VSLOTS, 0, :n] + tr[t % VSLOTS, 1, :n]
        xr[rows] = (xr[rows].astype(F32) + mlp).astype(BF16)

    def s_sent(k):
        t, n = k[0], k[3]
        left(sv.at[t % SSLOTS, pl.ds(0, n)], f_s.at[t % SSLOTS])
        left(sv.at[t % SSLOTS, pl.ds(0, 2 * n)], t_s.at[t % SSLOTS])

    def tick(t):
        def when(lag, f):
            @pl.when(jnp.logical_and(t >= lag, t < FULL + lag))
            def _():
                f(full(t - lag))

            @pl.when(t >= FULL + lag)
            def _():
                f(short(t - lag))

        def begin(k):
            def fetch():
                if k[3] == r:
                    @pl.when(t + 1 < FULL)
                    def _():
                        x_fetch(full(t + 1))

                    @pl.when(t + 1 == FULL)
                    def _():
                        x_fetch(short(t + 1))
                else:
                    @pl.when(t + 1 < TICKS)
                    def _():
                        x_fetch(short(t + 1))
            start(k, fetch, t == 0 if k[3] == r else None)
        when(3, sent)
        when(0, begin)
        when(1, relay)

        @pl.when(t == FULL + 3)
        def _():
            add_far(full(t - 4))

        @pl.when(t > FULL + 3)
        def _():
            add_far(short(t - 4))
        when(3, add_partner)

        @pl.when(t + 3 < J)
        def _():
            x_last(t + 3)
        when(4, p_sent)
        when(2, second)

        @pl.when(jnp.logical_and(t >= 4, t <= CATCH))
        def _():
            add_far(full(t - 4))

        @pl.when(jnp.logical_and(t >= CATCH, t < FULL + 2))
        def _():
            add_far(full(t - 3))
        when(5, finish)
        when(5, s_sent)
    loop(0, TICKS, tick)

    n4, n3, n2, n1 = (short(TICKS - i) for i in (4, 3, 2, 1))
    n5 = short(TICKS - 5)
    add_partner(n3)
    add_far(n4)
    p_sent(n4)
    relay(n1)
    second_early(n2)
    second_late(n2)
    p_sent(n3)
    finish(n5)
    s_sent(n5)
    add_far(n3)
    second_early(n1)
    add_partner(n2)
    second_late(n1)
    finish(n4)
    add_partner(n1)
    add_far(n2)
    finish(n3)
    add_far(n1)
    finish(n2)
    finish(n1)
    for k in (n3, n2, n1):
        sent(k)
    p_sent(n2)
    p_sent(n1)
    for k in (n4, n3, n2, n1):
        s_sent(k)

    left(gv.at[pl.ds(0, 3)], g_s)
    for part, (lo, hi) in enumerate(parts):
        left(w1v.at[pl.ds(0, 3 * KB), pl.ds(lo, hi - lo)], w1_s.at[part])
    left(x_ref, raw_s.at[0])
    left(x_ref, raw_s.at[1])
    rest = pl.ds(0, (J - 1) * half)
    left(x_ref.at[rest], raw_s.at[2])
    left(x_ref.at[rest], raw_s.at[3])
    left(x_ref.at[pl.ds(0, r)], raw_s.at[4])
    for i in (0, 1):
        left(xall_ref.at[pl.ds(0, J // 8)], x_s.at[i])
    for i in (2, 3):
        left(xall_ref.at[pl.ds(0, J // 16)], x_s.at[i])
    for i in range(4):
        left(xall_ref.at[pl.ds(0, J // 8)], d_s.at[i])


def solution(mesh):
    assert mesh.shape["tp2"] == RING and mesh.shape["tp"] == 2 * RING
    row_spec = P(("data", "tp"), "tp2")

    def local_block(x_loc, scale_loc, w_in_loc, w_out_loc):
        T, KB = x_loc.shape
        NB, DB = w_out_loc.shape
        NS, K, r = NB // RING, RING * KB, T // CHUNKS
        dma = pltpu.SemaphoreType.DMA
        any_spec = pl.BlockSpec(memory_space=pl.ANY)
        outs = pl.pallas_call(
            functools.partial(kernel, (T, KB, NS, DB, r)),
            out_shape=[
                pltpu.VMEM((T, DB), BF16),
                jax.ShapeDtypeStruct((RING, T, KB), BF16),
                jax.ShapeDtypeStruct((CHUNKS, 8, r, K), BF16),
            ],
            in_specs=[any_spec] * 4,
            out_specs=[pl.BlockSpec(memory_space=pltpu.VMEM), any_spec, any_spec],
            scratch_shapes=[
                pltpu.VMEM((K, NS), BF16),
                pltpu.VMEM((NB, DB), BF16),
                pltpu.VMEM((2, 8, r, K), BF16),
                pltpu.VMEM((HSLOTS, 8 * r, NB), BF16),
                pltpu.VMEM((SSLOTS, 4 * r, DB), F32),
                pltpu.VMEM((2, 4 * r, DB), F32),
                pltpu.VMEM((VSLOTS, 4 * r, DB), F32),
                pltpu.VMEM((FSLOTS, 2, r, DB // 2), F32),
                pltpu.VMEM((VSLOTS, 2, r, DB), F32),
                pltpu.VMEM((RING, 1, KB), F32),
                pltpu.VMEM((3, r, KB), BF16),
                pltpu.VMEM((r, K), BF16),
                dma, dma,
                dma((5,)), dma((RSLOTS, 2)),
                dma((2,)), dma((2,)),
                dma((4,)), dma((CHUNKS, 2)),
                dma((4,)), dma((CHUNKS,)),
                dma((HSLOTS,)), dma((HSLOTS, 2)), dma((HSLOTS,)),
                dma((2,)), dma((VSLOTS,)),
                dma((SSLOTS,)), dma((FSLOTS,)),
                dma((SSLOTS,)), dma((VSLOTS,)),
                dma((8,)), dma((2,)), dma,
            ],
            compiler_params=pltpu.CompilerParams(collective_id=0, has_side_effects=True, vmem_limit_bytes=60 * 2**20),
        )(x_loc, scale_loc.reshape(1, KB), w_in_loc, w_out_loc)
        return outs[0]

    return jax.shard_map(local_block, mesh=mesh, in_specs=(row_spec, P("tp2"), P("tp2", "tp"), P("tp", "tp2")), out_specs=row_spec, check_vma=False)
```

```python
import functools

import jax
import jax.numpy as jnp
from jax import lax
from jax.experimental import pallas as pl
from jax.experimental.pallas import tpu as pltpu
from jax.sharding import PartitionSpec as P

LN_EPS = 1e-6
RING = 4
CHUNKS = 16
FULL = 12
SPLIT = 2
TICKS = FULL + (CHUNKS - FULL) * SPLIT
FAR, NEAR, OWN = FULL, FULL + 2, FULL + 6
AHEAD = 4
CATCH = 8
RSLOTS, HSLOTS, SSLOTS, PSLOTS, VSLOTS, FSLOTS = 8, 5, 4, 2, 3, 4
MESH = pl.DeviceIdType.MESH
BF16, F32 = jnp.bfloat16, jnp.float32


def kernel(dims, x_ref, g_ref, w1_ref, w2_ref, xr, raw_ref, xall_ref, w1v, w2v, xv, hv, sv, pv, pr, hr, tr, hx, tx, gv,
           g_s, g_r, raw_s, raw_r, w1_s, w1_r, x_s, x_r, d_s, d_r, h_s, h_r, q_s, p_s, p_r, f_s, f_r, t_s, t_r, tx_r, l_s, xl_s, o_s):
    T, KB, NS, DB, r = dims
    J, K, small = CHUNKS, RING * KB, r // SPLIT
    half = r // 2
    d = lax.axis_index("data")
    y = lax.axis_index("tp2")
    tp = lax.axis_index("tp")
    x, c = tp // 2, tp % 2
    yp, yo, ym = (y + 1) % RING, (y + 2) % RING, (y + 3) % RING
    xp, xo, xm = (x + 1) % RING, (x + 2) % RING, (x + 3) % RING
    to_yp, to_ym, to_yo = (d, yp, tp), (d, ym, tp), (d, yo, tp)
    to_xp, to_xm = (d, y, xp * 2 + c), (d, y, xm * 2 + c)
    to_pt = (d, y, x * 2 + 1 - c)

    def rc(src, dst, ss, rs, dev):
        return pltpu.make_async_remote_copy(src_ref=src, dst_ref=dst, send_sem=ss, recv_sem=rs, device_id=dev, device_id_type=MESH)

    def arrived(ref, sem):
        rc(ref, ref, o_s, sem, to_pt).wait_recv()

    def left(ref, sem):
        rc(ref, ref, sem, o_s, to_pt).wait_send()

    def loop(lo, hi, f):
        def body(i, carry):
            f(i)
            return carry
        lax.fori_loop(lo, hi, body, 0)

    barrier = pltpu.get_barrier_semaphore()
    for dev in (to_yp, to_ym, to_yo, to_xp, to_xm, to_pt):
        pl.semaphore_signal(barrier, inc=1, device_id=dev, device_id_type=MESH)
    pl.semaphore_wait(barrier, 6)

    def raw_block(j, b):
        return raw_ref.at[b, pl.ds(pl.multiple_of(j * r, r), r)]

    def raw_own(j, dev, i, k=0):
        rows = pl.ds(pl.multiple_of(j * r, r), r)
        return rc(x_ref.at[rows], raw_ref.at[y, rows], raw_s.at[i], raw_r.at[j % RSLOTS, k], dev)

    def raw_relay(j, b, off, dev, i):
        part = raw_ref.at[b, pl.ds(pl.multiple_of(j * r + off, half), half)]
        return rc(part, part, raw_s.at[i], raw_r.at[j % RSLOTS, 1], dev)

    def send_raw(j):
        raw_own(j, to_yp, 0).start()
        raw_own(j, to_ym, 1).start()

    send_raw(0)
    raw_own(0, to_yo, 4, 1).start()
    gammas = [rc(g_ref, gv.at[y], g_s, g_r, dev) for dev in (to_yp, to_ym, to_yo)]
    for cp in gammas:
        cp.start()
    for j in range(1, AHEAD):
        send_raw(j)

    cut = NS * 4 // 7
    parts = ((0, cut), (cut, NS))

    def w1_block(b, part):
        lo, hi = parts[part]
        return w1v.at[pl.ds(pl.multiple_of(b * KB, KB), KB), pl.ds(lo, hi - lo)]

    def w1_copy(b, dev, part):
        lo, hi = parts[part]
        cols = w1_ref.at[:, pl.ds(pl.multiple_of(b * NS + lo, 128), hi - lo)]
        return rc(cols, w1_block(y, part), w1_s.at[part], w1_r.at[part], dev)

    def w1_wait(part):
        lo, hi = parts[part]
        arrived(w1v.at[pl.ds(0, 3 * KB), pl.ds(lo, hi - lo)], w1_r.at[part])

    own_g = pltpu.make_async_copy(g_ref, gv.at[y], l_s.at[3])
    own_x = pltpu.make_async_copy(x_ref, xr, l_s.at[4])
    own_w1 = pltpu.make_async_copy(w1_ref.at[:, pl.ds(pl.multiple_of(y * NS, 128), NS)], w1v.at[pl.ds(pl.multiple_of(y * KB, KB), KB)], l_s.at[5])
    own_w2 = pltpu.make_async_copy(w2_ref, w2v, l_s.at[6])
    own_g.start()
    own_x.start()
    own_w1.start()
    own_w2.start()

    def x_own(j, dev, i):
        return rc(xall_ref.at[j, x], xall_ref.at[j, x], x_s.at[i], x_r.at[j, 0], dev)

    def x_relay(j, b, off, dev, i):
        blk = xall_ref.at[j, b, pl.ds(off, half)]
        return rc(blk, blk, x_s.at[i], x_r.at[j, 1], dev)

    def d_copy(j, b, i):
        return rc(xall_ref.at[j, b], xall_ref.at[j, 4 + b], d_s.at[i], d_r.at[j], to_pt)

    def norm(j):
        arrived(raw_block(j, yo), raw_r.at[j % RSLOTS, 1])
        loads = [pltpu.make_async_copy(raw_block(j, b), xv.at[1, 1 + i, :, pl.ds(0, KB)], l_s.at[i]) for i, b in enumerate((yp, ym, yo))]
        for cp in loads:
            cp.start()
        for cp in loads:
            cp.wait()
        rows = pl.ds(pl.multiple_of(j * r, r), r)
        blocks = [(y, lambda: xr[rows]), (yp, lambda: xv[1, 1, :, :KB]), (ym, lambda: xv[1, 2, :, :KB]), (yo, lambda: xv[1, 3, :, :KB])]
        total = jnp.zeros((r, 1), F32)
        for _, get in blocks:
            total += jnp.sum(get().astype(F32), axis=1, keepdims=True)
        mean = total / K
        total = jnp.zeros((r, 1), F32)
        for _, get in blocks:
            dev = get().astype(F32) - mean
            total += jnp.sum(dev * dev, axis=1, keepdims=True)
        inv = lax.rsqrt(total / K + LN_EPS)
        for b, get in blocks:
            xv[1, 0, :, pl.ds(pl.multiple_of(b * KB, KB), KB)] = ((get().astype(F32) - mean) * inv * gv[b]).astype(BF16)
        out = pltpu.make_async_copy(xv.at[1, 0], xall_ref.at[j, x], l_s.at[7])
        out.start()
        out.wait()
        x_own(j, to_xp, 0).start()
        x_own(j, to_xm, 1).start()
        d_copy(j, x, 0).start()

    def x_step(j):
        arrived(xall_ref.at[j, pl.ds(0, 2)], x_r.at[j, 0])
        x_relay(j, xm, 0, to_xp, 2).start()
        x_relay(j, xp, half, to_xm, 3).start()
        d_copy(j, xp, 1).start()
        d_copy(j, xm, 2).start()

    def x_last(j):
        arrived(xall_ref.at[j, xo], x_r.at[j, 1])
        d_copy(j, xo, 3).start()

    def raw_wait(j):
        arrived(raw_ref.at[pl.ds(0, 2), pl.ds(0, r)], raw_r.at[j % RSLOTS, 0])

    def raw_step(j):
        raw_wait(j)
        raw_relay(j, ym, 0, to_yp, 2).start()
        raw_relay(j, yp, half, to_ym, 3).start()

    def raw_tick(j):
        raw_step(j)

        send_raw(j + AHEAD)

        @pl.when(jnp.logical_and(j >= 3, j < J - AHEAD))
        def _():
            norm(j - 2)

    own_x.wait()
    own_g.wait()
    raw_wait(0)
    send_raw(AHEAD)
    arrived(gv.at[pl.ds(0, 3)], g_r)
    norm(0)
    loop(1, J - AHEAD, raw_tick)
    loop(J - AHEAD, J, raw_step)
    w1_sends = [w1_copy(b, dev, part) for part in (0, 1) for b, dev in ((yp, to_yp), (ym, to_ym), (yo, to_yo))]
    for cp in w1_sends:
        cp.start()
    loop(J - AHEAD - 2, J, norm)
    loop(0, J, x_step)
    loop(0, 4, x_last)

    def full(t):
        return (t, t, 0, r)

    def short(t):
        return (t, FULL + (t - FULL) // SPLIT, (t - FULL) % SPLIT * small, small)

    def x_load(k):
        t, j = k[:2]
        return pltpu.make_async_copy(xall_ref.at[j], xv.at[t % 2], xl_s.at[t % 2])

    def x_piece(t, j, b, rows, i, to):
        pltpu.make_async_copy(xall_ref.at[j, b, rows], xv.at[t % 2, i, to], xl_s.at[t % 2]).start()

    def x_loaded(k):
        if k[3] == r:
            x_load(k).wait()
        else:
            half_slot = xv.at[k[0] % 2, pl.ds(0, 4)]
            pltpu.make_async_copy(xall_ref.at[0, pl.ds(0, 4)], half_slot, xl_s.at[k[0] % 2]).wait()

    def gathered(j):
        arrived(xall_ref.at[j, pl.ds(4, 4)], d_r.at[j])

    def fetch_full(t):
        gathered(t)
        x_load(full(t)).start()

    def fetch_owner(t):
        for i in (0, 1):
            @pl.when(t == FAR + i)
            def _():
                gathered(FULL + 2 * i)
                gathered(FULL + 2 * i + 1)
        every = pl.ds(0, r)
        order = {FAR + i: ((FULL + 2 * i, xo), (FULL + 2 * i + 1, xo)) for i in (0, 1)}
        order |= {NEAR + i: ((FULL + i, xp), (FULL + i, xm)) for i in range(4)}
        order |= {OWN + i: ((FULL + 2 * i, x), (FULL + 2 * i + 1, x)) for i in (0, 1)}
        for which, blocks in order.items():
            @pl.when(t == which)
            def _():
                for i, (j, b) in enumerate(blocks):
                    x_piece(t, j, b, every, i, every)
                    x_piece(t, j, 4 + b, every, 2 + i, every)

    fetch_full(0)
    own_w1.wait()
    own_w2.wait()
    w1_wait(0)

    def hcols(b, lo=0, hi=NS):
        return pl.ds(pl.multiple_of(b * NS + lo, 128), hi - lo)

    def h_own(k, dev, part):
        t, n = k[0], 8 * k[3]
        lo, hi = parts[part]
        blk = hv.at[t % HSLOTS, pl.ds(0, n), hcols(y, lo, hi)]
        return rc(blk, blk, h_s.at[t % HSLOTS], h_r.at[t % HSLOTS, 0], dev)

    def h_relay(k, b, side, dev):
        t, n = k[0], 4 * k[3]
        blk = hv.at[t % HSLOTS, pl.ds(side * n, n), hcols(b)]
        return rc(blk, blk, q_s.at[t % HSLOTS], h_r.at[t % HSLOTS, 1], dev)

    def h_bytes(k, blocks):
        return hv.at[k[0] % HSLOTS, pl.ds(0, 8 * k[3]), pl.ds(0, blocks * NS)]

    def sent(k):
        left(h_bytes(k, 2), h_s.at[k[0] % HSLOTS])
        left(h_bytes(k, 1), q_s.at[k[0] % HSLOTS])

    def start(k, fetch, first):
        t, n = k[0], k[3]
        x_loaded(k)
        fetch()
        for part, (lo, hi) in enumerate(parts):
            if part == 1 and first is not None:
                @pl.when(first)
                def _():
                    w1_wait(1)
            rows = xv[t % 2, :8 * n // r].reshape(8 * n, K)
            u = jnp.dot(rows, w1v[:, lo:hi], preferred_element_type=F32)
            hv[t % HSLOTS, :8 * n, hcols(y, lo, hi)] = jax.nn.gelu(u, approximate=True).astype(BF16)
            h_own(k, to_yp, part).start()
            h_own(k, to_ym, part).start()

    def relay(k):
        arrived(h_bytes(k, 2), h_r.at[k[0] % HSLOTS, 0])
        h_relay(k, ym, 0, to_yp).start()
        h_relay(k, yp, 1, to_ym).start()

    def p_copy(k):
        t, n = k[0], 4 * k[3]
        return rc(pv.at[t % 2, pl.ds(0, n)], pr.at[t % PSLOTS, pl.ds(0, n)], p_s.at[t % 2], p_r.at[t % PSLOTS], to_pt)

    def p_sent(k):
        p_copy(k).wait_send()

    def second(k):
        t, n = k[0], 4 * k[3]
        arrived(h_bytes(k, 1), h_r.at[t % HSLOTS, 1])
        tn = DB // 2

        def cols(i):
            o = pl.ds(pl.multiple_of(i * tn, tn), tn)
            u = jnp.dot(hv[t % HSLOTS, :2 * n], w2v[:, o], preferred_element_type=F32)
            sv[t % SSLOTS, :n, o] = u[:n]
            pv[t % 2, :n, o] = u[n:]
        loop(0, 2, cols)
        p_copy(k).start()

    def second_part(k, blocks, add):
        t, n = k[0], 4 * k[3]
        tn = DB // 2

        def cols(i):
            o = pl.ds(pl.multiple_of(i * tn, tn), tn)
            u = sum(jnp.dot(hv[t % HSLOTS, :2 * n, hcols(b)], w2v[pl.ds(pl.multiple_of(b * NS, NS), NS), o], preferred_element_type=F32) for b in blocks)
            if add:
                sv[t % SSLOTS, :n, o] += u[:n]
                pv[t % 2, :n, o] += u[n:]
            else:
                sv[t % SSLOTS, :n, o] = u[:n]
                pv[t % 2, :n, o] = u[n:]
        loop(0, 2, cols)

    def second_early(k):
        second_part(k, (y, yp, ym), False)

    def second_late(k):
        arrived(h_bytes(k, 1), h_r.at[k[0] % HSLOTS, 1])
        second_part(k, (yo,), True)
        p_copy(k).start()

    def s_rows(k, b):
        return pl.ds(pl.multiple_of(b * k[3], k[3]), k[3])

    def f_copy(k, side, dev):
        t, n = k[0], k[3]
        cols = pl.ds(side * (DB // 2), DB // 2)
        return rc(sv.at[t % SSLOTS, s_rows(k, xo), cols], hr.at[t % FSLOTS, side, pl.ds(0, n)], f_s.at[t % SSLOTS], f_r.at[t % FSLOTS], dev)

    def t_copy(k, b, dev, q):
        t, n = k[0], k[3]
        return rc(sv.at[t % SSLOTS, s_rows(k, b)], tr.at[t % VSLOTS, q, pl.ds(0, n)], t_s.at[t % SSLOTS], t_r.at[t % VSLOTS], dev)

    def add_core(k):
        t, n = k[0], 4 * k[3]
        p_copy(k).wait_recv()
        sv[t % SSLOTS, :n] += pr[t % PSLOTS, :n]

    def add_partner(k):
        add_core(k)
        f_copy(k, 0, to_xp).start()
        f_copy(k, 1, to_xm).start()

    def add_far(k):
        t, n = k[0], k[3]
        m = DB // 2
        arrived(hr.at[t % FSLOTS, :, pl.ds(0, n)], f_r.at[t % FSLOTS])
        sv[t % SSLOTS, s_rows(k, xp), :m] += hr[t % FSLOTS, 0, :n]
        sv[t % SSLOTS, s_rows(k, xm), m:] += hr[t % FSLOTS, 1, :n]
        t_copy(k, xp, to_xp, 1).start()
        t_copy(k, xm, to_xm, 0).start()

    def finish(k):
        t, j, off, n = k
        arrived(tr.at[t % VSLOTS, :, pl.ds(0, n)], t_r.at[t % VSLOTS])
        rows = pl.ds(pl.multiple_of(j * r + off, n), n)
        mlp = sv[t % SSLOTS, s_rows(k, x)] + tr[t % VSLOTS, 0, :n] + tr[t % VSLOTS, 1, :n]
        xr[rows] = (xr[rows].astype(F32) + mlp).astype(BF16)

    def s_sent(k):
        t, n = k[0], k[3]
        left(sv.at[t % SSLOTS, pl.ds(0, n)], f_s.at[t % SSLOTS])
        left(sv.at[t % SSLOTS, pl.ds(0, 2 * n)], t_s.at[t % SSLOTS])

    def send_far(i):
        t = FAR + i
        add_core(short(t))
        for side, dev in ((0, to_xp), (1, to_xm)):
            src = sv.at[t % SSLOTS, pl.ds(0, 2 * r), pl.ds(side * (DB // 2), DB // 2)]
            rc(src, hx.at[i, side], f_s.at[t % SSLOTS], f_r.at[t % FSLOTS], dev).start()

    def send_near(i):
        t = NEAR + i
        add_core(short(t))
        if i % 2 == 0:
            arrived(hx.at[i // 2], f_r.at[(FAR + i // 2) % FSLOTS])
        m, slot, rows = DB // 2, t % SSLOTS, pl.ds(i % 2 * r, r)
        sv[slot, :r, :m] += hx[i // 2, 0, rows]
        sv[slot, r:2 * r, m:] += hx[i // 2, 1, rows]
        rc(sv.at[slot, pl.ds(0, r)], tx.at[i, 1], t_s.at[slot], tx_r.at[i], to_xp).start()
        rc(sv.at[slot, pl.ds(r, r)], tx.at[i, 0], t_s.at[slot], tx_r.at[i], to_xm).start()

    def finish_own(i):
        t = OWN + i
        for h in (0, 1):
            q = 2 * i + h
            arrived(tx.at[q], tx_r.at[q])
            rows = pl.ds((FULL + q) * r, r)
            mlp = sv[t % SSLOTS, h * r:(h + 1) * r] + tx[q, 0] + tx[q, 1]
            xr[rows] = (xr[rows].astype(F32) + mlp).astype(BF16)

    def two_rows_left(sem):
        left(sv.at[0, pl.ds(0, 2 * r)], sem)

    def tick(t):
        def when(lag, f, until=TICKS):
            @pl.when(jnp.logical_and(t >= lag, t < FULL + lag))
            def _():
                f(full(t - lag))

            if until > FULL:
                @pl.when(jnp.logical_and(t >= FULL + lag, t < until + lag))
                def _():
                    f(short(t - lag))

        def begin(k):
            def fetch():
                if k[3] == r:
                    @pl.when(t + 1 < FULL)
                    def _():
                        fetch_full(t + 1)

                    @pl.when(t + 1 == FULL)
                    def _():
                        fetch_owner(t + 1)
                else:
                    @pl.when(t + 1 < TICKS)
                    def _():
                        fetch_owner(t + 1)
            start(k, fetch, t == 0 if k[3] == r else None)
        when(3, sent)
        when(0, begin)
        when(1, relay)

        for i in (0, 1):
            @pl.when(t == FAR + i + 3)
            def _():
                send_far(i)

        for i in (0, 1, 2):
            @pl.when(t == NEAR + i + 3)
            def _():
                send_near(i)

        @pl.when(t == FULL + 3)
        def _():
            add_far(full(t - 4))

        when(3, add_partner, FULL)

        @pl.when(t + 4 < J)
        def _():
            x_last(t + 4)
        when(4, p_sent)
        when(2, second)

        @pl.when(jnp.logical_and(t >= 4, t <= CATCH))
        def _():
            add_far(full(t - 4))

        @pl.when(jnp.logical_and(t >= CATCH, t < FULL + 2))
        def _():
            add_far(full(t - 3))
        when(5, finish, FULL)
        when(5, s_sent, FULL)

        for i in (0, 1):
            @pl.when(t == FAR + i + 5)
            def _():
                two_rows_left(f_s.at[(FAR + i) % SSLOTS])
    loop(0, TICKS, tick)

    n4, n3, n2, n1 = (short(TICKS - i) for i in (4, 3, 2, 1))
    send_near(3)
    p_sent(n4)
    two_rows_left(t_s.at[NEAR % SSLOTS])
    relay(n1)
    second_early(n2)
    second_late(n2)
    p_sent(n3)
    two_rows_left(t_s.at[(NEAR + 1) % SSLOTS])
    second_early(n1)
    add_core(n2)
    second_late(n1)
    finish_own(0)
    add_core(n1)
    finish_own(1)
    for k in (n3, n2, n1):
        sent(k)
    p_sent(n2)
    p_sent(n1)
    two_rows_left(t_s.at[(NEAR + 2) % SSLOTS])
    two_rows_left(t_s.at[(NEAR + 3) % SSLOTS])

    left(gv.at[pl.ds(0, 3)], g_s)
    for part, (lo, hi) in enumerate(parts):
        left(w1v.at[pl.ds(0, 3 * KB), pl.ds(lo, hi - lo)], w1_s.at[part])
    left(x_ref, raw_s.at[0])
    left(x_ref, raw_s.at[1])
    rest = pl.ds(0, (J - 1) * half)
    left(x_ref.at[rest], raw_s.at[2])
    left(x_ref.at[rest], raw_s.at[3])
    left(x_ref.at[pl.ds(0, r)], raw_s.at[4])
    for i in (0, 1):
        left(xall_ref.at[pl.ds(0, J // 8)], x_s.at[i])
    for i in (2, 3):
        left(xall_ref.at[pl.ds(0, J // 16)], x_s.at[i])
    for i in range(4):
        left(xall_ref.at[pl.ds(0, J // 8)], d_s.at[i])


def solution(mesh):
    assert mesh.shape["tp2"] == RING and mesh.shape["tp"] == 2 * RING
    row_spec = P(("data", "tp"), "tp2")

    def local_block(x_loc, scale_loc, w_in_loc, w_out_loc):
        T, KB = x_loc.shape
        NB, DB = w_out_loc.shape
        NS, K, r = NB // RING, RING * KB, T // CHUNKS
        dma = pltpu.SemaphoreType.DMA
        any_spec = pl.BlockSpec(memory_space=pl.ANY)
        outs = pl.pallas_call(
            functools.partial(kernel, (T, KB, NS, DB, r)),
            out_shape=[
                pltpu.VMEM((T, DB), BF16),
                jax.ShapeDtypeStruct((RING, T, KB), BF16),
                jax.ShapeDtypeStruct((CHUNKS, 8, r, K), BF16),
            ],
            in_specs=[any_spec] * 4,
            out_specs=[pl.BlockSpec(memory_space=pltpu.VMEM), any_spec, any_spec],
            scratch_shapes=[
                pltpu.VMEM((K, NS), BF16),
                pltpu.VMEM((NB, DB), BF16),
                pltpu.VMEM((2, 8, r, K), BF16),
                pltpu.VMEM((HSLOTS, 8 * r, NB), BF16),
                pltpu.VMEM((SSLOTS, 4 * r, DB), F32),
                pltpu.VMEM((2, 4 * r, DB), F32),
                pltpu.VMEM((PSLOTS, 4 * r, DB), F32),
                pltpu.VMEM((FSLOTS, 2, r, DB // 2), F32),
                pltpu.VMEM((VSLOTS, 2, r, DB), F32),
                pltpu.VMEM((2, 2, 2 * r, DB // 2), F32),
                pltpu.VMEM((4, 2, r, DB), F32),
                pltpu.VMEM((RING, 1, KB), F32),
                dma, dma,
                dma((5,)), dma((RSLOTS, 2)),
                dma((2,)), dma((2,)),
                dma((4,)), dma((CHUNKS, 2)),
                dma((4,)), dma((CHUNKS,)),
                dma((HSLOTS,)), dma((HSLOTS, 2)), dma((HSLOTS,)),
                dma((2,)), dma((PSLOTS,)),
                dma((SSLOTS,)), dma((FSLOTS,)),
                dma((SSLOTS,)), dma((VSLOTS,)), dma((4,)),
                dma((8,)), dma((2,)), dma,
            ],
            compiler_params=pltpu.CompilerParams(collective_id=0, has_side_effects=True, vmem_limit_bytes=61 * 2**20 + 3 * 2**18),
        )(x_loc, scale_loc.reshape(1, KB), w_in_loc, w_out_loc)
        return outs[0]

    return jax.shard_map(local_block, mesh=mesh, in_specs=(row_spec, P("tp2"), P("tp2", "tp"), P("tp", "tp2")), out_specs=row_spec, check_vma=False)
```

```python
import functools

import jax
import jax.numpy as jnp
from jax import lax
from jax.experimental import pallas as pl
from jax.experimental.pallas import tpu as pltpu
from jax.sharding import PartitionSpec as P

LN_EPS = 1e-6
RING = 4
CHUNKS = 16
FULL = 12
SPLIT = 2
TICKS = FULL + (CHUNKS - FULL) * SPLIT
FAR, NEAR, OWN = FULL, FULL + 2, FULL + 6
AHEAD = 4
CATCH = 8
RSLOTS, HSLOTS, SSLOTS, PSLOTS, VSLOTS, FSLOTS = 8, 5, 4, 2, 3, 4
MESH = pl.DeviceIdType.MESH
BF16, F32 = jnp.bfloat16, jnp.float32


def kernel(dims, x_ref, g_ref, w1_ref, w2_ref, xr, raw_ref, xall_ref, w1v, w2v, xv, hv, sv, pv, pr, hr, tr, hx, tx, gv,
           g_s, g_r, raw_s, raw_r, w1_s, w1_r, x_s, x_r, d_s, d_r, h_s, h_r, q_s, p_s, p_r, f_s, f_r, t_s, t_r, tx_r, l_s, xl_s, o_s):
    T, KB, NS, DB, r = dims
    J, K, small = CHUNKS, RING * KB, r // SPLIT
    half = r // 2
    d = lax.axis_index("data")
    y = lax.axis_index("tp2")
    tp = lax.axis_index("tp")
    x, c = tp // 2, tp % 2
    yp, yo, ym = (y + 1) % RING, (y + 2) % RING, (y + 3) % RING
    xp, xo, xm = (x + 1) % RING, (x + 2) % RING, (x + 3) % RING
    to_yp, to_ym, to_yo = (d, yp, tp), (d, ym, tp), (d, yo, tp)
    to_xp, to_xm = (d, y, xp * 2 + c), (d, y, xm * 2 + c)
    to_pt = (d, y, x * 2 + 1 - c)

    def rc(src, dst, ss, rs, dev):
        return pltpu.make_async_remote_copy(src_ref=src, dst_ref=dst, send_sem=ss, recv_sem=rs, device_id=dev, device_id_type=MESH)

    def arrived(ref, sem):
        rc(ref, ref, o_s, sem, to_pt).wait_recv()

    def left(ref, sem):
        rc(ref, ref, sem, o_s, to_pt).wait_send()

    def loop(lo, hi, f):
        def body(i, carry):
            f(i)
            return carry
        lax.fori_loop(lo, hi, body, 0)

    barrier = pltpu.get_barrier_semaphore()
    for dev in (to_yp, to_ym, to_yo, to_xp, to_xm, to_pt):
        pl.semaphore_signal(barrier, inc=1, device_id=dev, device_id_type=MESH)
    pl.semaphore_wait(barrier, 6)

    def raw_block(j, b):
        return raw_ref.at[b, pl.ds(pl.multiple_of(j * r, r), r)]

    def raw_own(j, dev, i, k=0):
        rows = pl.ds(pl.multiple_of(j * r, r), r)
        return rc(x_ref.at[rows], raw_ref.at[y, rows], raw_s.at[i], raw_r.at[j % RSLOTS, k], dev)

    def raw_relay(j, b, off, dev, i):
        part = raw_ref.at[b, pl.ds(pl.multiple_of(j * r + off, half), half)]
        return rc(part, part, raw_s.at[i], raw_r.at[j % RSLOTS, 1], dev)

    def send_raw(j):
        raw_own(j, to_yp, 0).start()
        raw_own(j, to_ym, 1).start()

    send_raw(0)
    raw_own(0, to_yo, 4, 1).start()
    gammas = [rc(g_ref, gv.at[y], g_s, g_r, dev) for dev in (to_yp, to_ym, to_yo)]
    for cp in gammas:
        cp.start()
    for j in range(1, AHEAD):
        send_raw(j)

    cut = NS * 4 // 7
    parts = ((0, cut), (cut, NS))

    def w1_block(b, part):
        lo, hi = parts[part]
        return w1v.at[pl.ds(pl.multiple_of(b * KB, KB), KB), pl.ds(lo, hi - lo)]

    def w1_copy(b, dev, part):
        lo, hi = parts[part]
        cols = w1_ref.at[:, pl.ds(pl.multiple_of(b * NS + lo, 128), hi - lo)]
        return rc(cols, w1_block(y, part), w1_s.at[part], w1_r.at[part], dev)

    def w1_wait(part):
        lo, hi = parts[part]
        arrived(w1v.at[pl.ds(0, 3 * KB), pl.ds(lo, hi - lo)], w1_r.at[part])

    own_g = pltpu.make_async_copy(g_ref, gv.at[y], l_s.at[3])
    own_x = pltpu.make_async_copy(x_ref, xr, l_s.at[4])
    own_w1 = pltpu.make_async_copy(w1_ref.at[:, pl.ds(pl.multiple_of(y * NS, 128), NS)], w1v.at[pl.ds(pl.multiple_of(y * KB, KB), KB)], l_s.at[5])
    own_w2 = pltpu.make_async_copy(w2_ref, w2v, l_s.at[6])
    own_g.start()
    own_x.start()
    own_w1.start()
    own_w2.start()

    def x_own(j, dev, i):
        return rc(xall_ref.at[j, x], xall_ref.at[j, x], x_s.at[i], x_r.at[j, 0], dev)

    def x_relay(j, b, off, dev, i):
        blk = xall_ref.at[j, b, pl.ds(off, half)]
        return rc(blk, blk, x_s.at[i], x_r.at[j, 1], dev)

    def d_copy(j, b, i):
        return rc(xall_ref.at[j, b], xall_ref.at[j, 4 + b], d_s.at[i], d_r.at[j], to_pt)

    def norm(j):
        arrived(raw_block(j, yo), raw_r.at[j % RSLOTS, 1])
        loads = [pltpu.make_async_copy(raw_block(j, b), xv.at[1, 1 + i, :, pl.ds(0, KB)], l_s.at[i]) for i, b in enumerate((yp, ym, yo))]
        for cp in loads:
            cp.start()
        for cp in loads:
            cp.wait()
        rows = pl.ds(pl.multiple_of(j * r, r), r)
        blocks = [(y, lambda: xr[rows]), (yp, lambda: xv[1, 1, :, :KB]), (ym, lambda: xv[1, 2, :, :KB]), (yo, lambda: xv[1, 3, :, :KB])]
        total = jnp.zeros((r, 1), F32)
        for _, get in blocks:
            total += jnp.sum(get().astype(F32), axis=1, keepdims=True)
        mean = total / K
        total = jnp.zeros((r, 1), F32)
        for _, get in blocks:
            dev = get().astype(F32) - mean
            total += jnp.sum(dev * dev, axis=1, keepdims=True)
        inv = lax.rsqrt(total / K + LN_EPS)
        for b, get in blocks:
            xv[1, 0, :, pl.ds(pl.multiple_of(b * KB, KB), KB)] = ((get().astype(F32) - mean) * inv * gv[b]).astype(BF16)
        out = pltpu.make_async_copy(xv.at[1, 0], xall_ref.at[j, x], l_s.at[7])
        out.start()
        out.wait()
        x_own(j, to_xp, 0).start()
        x_own(j, to_xm, 1).start()
        d_copy(j, x, 0).start()

    def x_step(j):
        arrived(xall_ref.at[j, pl.ds(0, 2)], x_r.at[j, 0])
        x_relay(j, xm, 0, to_xp, 2).start()
        x_relay(j, xp, half, to_xm, 3).start()
        d_copy(j, xp, 1).start()
        d_copy(j, xm, 2).start()

    def x_last(j):
        arrived(xall_ref.at[j, xo], x_r.at[j, 1])
        d_copy(j, xo, 3).start()

    def raw_wait(j):
        arrived(raw_ref.at[pl.ds(0, 2), pl.ds(0, r)], raw_r.at[j % RSLOTS, 0])

    def raw_step(j):
        raw_wait(j)
        raw_relay(j, ym, 0, to_yp, 2).start()
        raw_relay(j, yp, half, to_ym, 3).start()

    def raw_tick(j):
        raw_step(j)

        send_raw(j + AHEAD)

        @pl.when(jnp.logical_and(j >= 3, j < J - AHEAD))
        def _():
            norm(j - 2)

    own_x.wait()
    own_g.wait()
    raw_wait(0)
    send_raw(AHEAD)
    arrived(gv.at[pl.ds(0, 3)], g_r)
    norm(0)
    loop(1, J - AHEAD, raw_tick)
    loop(J - AHEAD, J, raw_step)
    w1_sends = [w1_copy(b, dev, part) for part in (0, 1) for b, dev in ((yp, to_yp), (ym, to_ym), (yo, to_yo))]
    for cp in w1_sends:
        cp.start()
    loop(J - AHEAD - 2, J, norm)
    loop(0, J, x_step)
    loop(0, 4, x_last)

    def full(t):
        return (t, t, 0, r)

    def short(t):
        return (t, FULL + (t - FULL) // SPLIT, (t - FULL) % SPLIT * small, small)

    def x_load(k):
        t, j = k[:2]
        return pltpu.make_async_copy(xall_ref.at[j], xv.at[t % 2], xl_s.at[t % 2])

    def x_piece(t, j, b, rows, i, to):
        pltpu.make_async_copy(xall_ref.at[j, b, rows], xv.at[t % 2, i, to], xl_s.at[t % 2]).start()

    def x_loaded(k):
        if k[3] == r:
            x_load(k).wait()
        else:
            half_slot = xv.at[k[0] % 2, pl.ds(0, 4)]
            pltpu.make_async_copy(xall_ref.at[0, pl.ds(0, 4)], half_slot, xl_s.at[k[0] % 2]).wait()

    def gathered(j):
        arrived(xall_ref.at[j, pl.ds(4, 4)], d_r.at[j])

    def fetch_full(t):
        gathered(t)
        x_load(full(t)).start()

    def fetch_owner(t):
        for i in (0, 1):
            @pl.when(t == FAR + i)
            def _():
                gathered(FULL + 2 * i)
                gathered(FULL + 2 * i + 1)
        every = pl.ds(0, r)
        order = {FAR + i: ((FULL + 2 * i, xo), (FULL + 2 * i + 1, xo)) for i in (0, 1)}
        order |= {NEAR + i: ((FULL + i, xp), (FULL + i, xm)) for i in range(4)}
        order |= {OWN + i: ((FULL + 2 * i, x), (FULL + 2 * i + 1, x)) for i in (0, 1)}
        for which, blocks in order.items():
            @pl.when(t == which)
            def _():
                for i, (j, b) in enumerate(blocks):
                    x_piece(t, j, b, every, i, every)
                    x_piece(t, j, 4 + b, every, 2 + i, every)

    fetch_full(0)
    own_w1.wait()
    own_w2.wait()
    w1_wait(0)

    def hcols(b, lo=0, hi=NS):
        return pl.ds(pl.multiple_of(b * NS + lo, 128), hi - lo)

    def h_own(k, dev, part):
        t, n = k[0], 8 * k[3]
        lo, hi = parts[part]
        blk = hv.at[t % HSLOTS, pl.ds(0, n), hcols(y, lo, hi)]
        return rc(blk, blk, h_s.at[t % HSLOTS], h_r.at[t % HSLOTS, 0], dev)

    def h_relay(k, b, side, dev):
        t, n = k[0], 4 * k[3]
        blk = hv.at[t % HSLOTS, pl.ds(side * n, n), hcols(b)]
        return rc(blk, blk, q_s.at[t % HSLOTS], h_r.at[t % HSLOTS, 1], dev)

    def h_bytes(k, blocks):
        return hv.at[k[0] % HSLOTS, pl.ds(0, 8 * k[3]), pl.ds(0, blocks * NS)]

    def sent(k):
        left(h_bytes(k, 2), h_s.at[k[0] % HSLOTS])
        left(h_bytes(k, 1), q_s.at[k[0] % HSLOTS])

    def start(k, fetch, first):
        t, n = k[0], k[3]
        x_loaded(k)
        fetch()
        for part, (lo, hi) in enumerate(parts):
            if part == 1 and first is not None:
                @pl.when(first)
                def _():
                    w1_wait(1)
            rows = xv[t % 2, :8 * n // r].reshape(8 * n, K)
            u = jnp.dot(rows, w1v[:, lo:hi], preferred_element_type=F32)
            hv[t % HSLOTS, :8 * n, hcols(y, lo, hi)] = jax.nn.gelu(u, approximate=True).astype(BF16)
            h_own(k, to_yp, part).start()
            h_own(k, to_ym, part).start()

    def relay(k):
        arrived(h_bytes(k, 2), h_r.at[k[0] % HSLOTS, 0])
        h_relay(k, ym, 0, to_yp).start()
        h_relay(k, yp, 1, to_ym).start()

    def p_copy(k):
        t, n = k[0], 4 * k[3]
        return rc(pv.at[t % 2, pl.ds(0, n)], pr.at[t % PSLOTS, pl.ds(0, n)], p_s.at[t % 2], p_r.at[t % PSLOTS], to_pt)

    def p_sent(k):
        p_copy(k).wait_send()

    def second(k):
        t, n = k[0], 4 * k[3]
        arrived(h_bytes(k, 1), h_r.at[t % HSLOTS, 1])
        tn = DB // 2

        def cols(i):
            o = pl.ds(pl.multiple_of(i * tn, tn), tn)
            u = jnp.dot(hv[t % HSLOTS, :2 * n], w2v[:, o], preferred_element_type=F32)
            sv[t % SSLOTS, :n, o] = u[:n]
            pv[t % 2, :n, o] = u[n:]
        loop(0, 2, cols)
        p_copy(k).start()

    def second_part(k, blocks, add):
        t, n = k[0], 4 * k[3]
        tn = DB // 2

        def cols(i):
            o = pl.ds(pl.multiple_of(i * tn, tn), tn)
            u = sum(jnp.dot(hv[t % HSLOTS, :2 * n, hcols(b)], w2v[pl.ds(pl.multiple_of(b * NS, NS), NS), o], preferred_element_type=F32) for b in blocks)
            if add:
                sv[t % SSLOTS, :n, o] += u[:n]
                pv[t % 2, :n, o] += u[n:]
                rc(pv.at[t % 2, pl.ds(0, n), o], pr.at[t % PSLOTS, pl.ds(0, n), o], p_s.at[t % 2], p_r.at[t % PSLOTS], to_pt).start()
            else:
                sv[t % SSLOTS, :n, o] = u[:n]
                pv[t % 2, :n, o] = u[n:]
        loop(0, 2, cols)

    def second_early(k):
        second_part(k, (y, yp, ym), False)

    def second_late(k):
        arrived(h_bytes(k, 1), h_r.at[k[0] % HSLOTS, 1])
        second_part(k, (yo,), True)

    def s_rows(k, b):
        return pl.ds(pl.multiple_of(b * k[3], k[3]), k[3])

    def f_copy(k, side, dev):
        t, n = k[0], k[3]
        cols = pl.ds(side * (DB // 2), DB // 2)
        return rc(sv.at[t % SSLOTS, s_rows(k, xo), cols], hr.at[t % FSLOTS, side, pl.ds(0, n)], f_s.at[t % SSLOTS], f_r.at[t % FSLOTS], dev)

    def t_copy(k, b, dev, q):
        t, n = k[0], k[3]
        return rc(sv.at[t % SSLOTS, s_rows(k, b)], tr.at[t % VSLOTS, q, pl.ds(0, n)], t_s.at[t % SSLOTS], t_r.at[t % VSLOTS], dev)

    def add_core(k):
        t, n = k[0], 4 * k[3]
        p_copy(k).wait_recv()
        sv[t % SSLOTS, :n] += pr[t % PSLOTS, :n]

    def add_partner(k):
        add_core(k)
        f_copy(k, 0, to_xp).start()
        f_copy(k, 1, to_xm).start()

    def add_far(k):
        t, n = k[0], k[3]
        m = DB // 2
        arrived(hr.at[t % FSLOTS, :, pl.ds(0, n)], f_r.at[t % FSLOTS])
        sv[t % SSLOTS, s_rows(k, xp), :m] += hr[t % FSLOTS, 0, :n]
        sv[t % SSLOTS, s_rows(k, xm), m:] += hr[t % FSLOTS, 1, :n]
        t_copy(k, xp, to_xp, 1).start()
        t_copy(k, xm, to_xm, 0).start()

    def finish(k):
        t, j, off, n = k
        arrived(tr.at[t % VSLOTS, :, pl.ds(0, n)], t_r.at[t % VSLOTS])
        rows = pl.ds(pl.multiple_of(j * r + off, n), n)
        mlp = sv[t % SSLOTS, s_rows(k, x)] + tr[t % VSLOTS, 0, :n] + tr[t % VSLOTS, 1, :n]
        xr[rows] = (xr[rows].astype(F32) + mlp).astype(BF16)

    def s_sent(k):
        t, n = k[0], k[3]
        left(sv.at[t % SSLOTS, pl.ds(0, n)], f_s.at[t % SSLOTS])
        left(sv.at[t % SSLOTS, pl.ds(0, 2 * n)], t_s.at[t % SSLOTS])

    def send_far(i):
        t = FAR + i
        add_core(short(t))
        for side, dev in ((0, to_xp), (1, to_xm)):
            src = sv.at[t % SSLOTS, pl.ds(0, 2 * r), pl.ds(side * (DB // 2), DB // 2)]
            rc(src, hx.at[i, side], f_s.at[t % SSLOTS], f_r.at[t % FSLOTS], dev).start()

    def send_near(i):
        t = NEAR + i
        add_core(short(t))
        if i % 2 == 0:
            arrived(hx.at[i // 2], f_r.at[(FAR + i // 2) % FSLOTS])
        m, slot, rows = DB // 2, t % SSLOTS, pl.ds(i % 2 * r, r)
        sv[slot, :r, :m] += hx[i // 2, 0, rows]
        sv[slot, r:2 * r, m:] += hx[i // 2, 1, rows]
        rc(sv.at[slot, pl.ds(0, r)], tx.at[i, 1], t_s.at[slot], tx_r.at[i], to_xp).start()
        rc(sv.at[slot, pl.ds(r, r)], tx.at[i, 0], t_s.at[slot], tx_r.at[i], to_xm).start()

    def finish_own(i):
        t = OWN + i
        for h in (0, 1):
            q = 2 * i + h
            arrived(tx.at[q], tx_r.at[q])
            rows = pl.ds((FULL + q) * r, r)
            mlp = sv[t % SSLOTS, h * r:(h + 1) * r] + tx[q, 0] + tx[q, 1]
            xr[rows] = (xr[rows].astype(F32) + mlp).astype(BF16)

    def two_rows_left(sem):
        left(sv.at[0, pl.ds(0, 2 * r)], sem)

    def tick(t):
        def when(lag, f, until=TICKS):
            @pl.when(jnp.logical_and(t >= lag, t < FULL + lag))
            def _():
                f(full(t - lag))

            if until > FULL:
                @pl.when(jnp.logical_and(t >= FULL + lag, t < until + lag))
                def _():
                    f(short(t - lag))

        def begin(k):
            def fetch():
                if k[3] == r:
                    @pl.when(t + 1 < FULL)
                    def _():
                        fetch_full(t + 1)

                    @pl.when(t + 1 == FULL)
                    def _():
                        fetch_owner(t + 1)
                else:
                    @pl.when(t + 1 < TICKS)
                    def _():
                        fetch_owner(t + 1)
            start(k, fetch, t == 0 if k[3] == r else None)
        when(3, sent)
        when(0, begin)
        when(1, relay)

        for i in (0, 1):
            @pl.when(t == FAR + i + 3)
            def _():
                send_far(i)

        for i in (0, 1, 2):
            @pl.when(t == NEAR + i + 3)
            def _():
                send_near(i)

        @pl.when(t == FULL + 3)
        def _():
            add_far(full(t - 4))

        when(3, add_partner, FULL)

        @pl.when(t + 4 < J)
        def _():
            x_last(t + 4)
        when(4, p_sent)
        when(2, second)

        @pl.when(jnp.logical_and(t >= 4, t <= CATCH))
        def _():
            add_far(full(t - 4))

        @pl.when(jnp.logical_and(t >= CATCH, t < FULL + 2))
        def _():
            add_far(full(t - 3))
        when(5, finish, FULL)
        when(5, s_sent, FULL)

        for i in (0, 1):
            @pl.when(t == FAR + i + 5)
            def _():
                two_rows_left(f_s.at[(FAR + i) % SSLOTS])
    loop(0, TICKS, tick)

    n4, n3, n2, n1 = (short(TICKS - i) for i in (4, 3, 2, 1))
    send_near(3)
    p_sent(n4)
    two_rows_left(t_s.at[NEAR % SSLOTS])
    relay(n1)
    second_early(n2)
    second_late(n2)
    p_sent(n3)
    two_rows_left(t_s.at[(NEAR + 1) % SSLOTS])
    second_early(n1)
    add_core(n2)
    second_late(n1)
    finish_own(0)
    add_core(n1)
    finish_own(1)
    for k in (n3, n2, n1):
        sent(k)
    p_sent(n2)
    p_sent(n1)
    two_rows_left(t_s.at[(NEAR + 2) % SSLOTS])
    two_rows_left(t_s.at[(NEAR + 3) % SSLOTS])

    left(gv.at[pl.ds(0, 3)], g_s)
    for part, (lo, hi) in enumerate(parts):
        left(w1v.at[pl.ds(0, 3 * KB), pl.ds(lo, hi - lo)], w1_s.at[part])
    left(x_ref, raw_s.at[0])
    left(x_ref, raw_s.at[1])
    rest = pl.ds(0, (J - 1) * half)
    left(x_ref.at[rest], raw_s.at[2])
    left(x_ref.at[rest], raw_s.at[3])
    left(x_ref.at[pl.ds(0, r)], raw_s.at[4])
    for i in (0, 1):
        left(xall_ref.at[pl.ds(0, J // 8)], x_s.at[i])
    for i in (2, 3):
        left(xall_ref.at[pl.ds(0, J // 16)], x_s.at[i])
    for i in range(4):
        left(xall_ref.at[pl.ds(0, J // 8)], d_s.at[i])


def solution(mesh):
    assert mesh.shape["tp2"] == RING and mesh.shape["tp"] == 2 * RING
    row_spec = P(("data", "tp"), "tp2")

    def local_block(x_loc, scale_loc, w_in_loc, w_out_loc):
        T, KB = x_loc.shape
        NB, DB = w_out_loc.shape
        NS, K, r = NB // RING, RING * KB, T // CHUNKS
        dma = pltpu.SemaphoreType.DMA
        any_spec = pl.BlockSpec(memory_space=pl.ANY)
        outs = pl.pallas_call(
            functools.partial(kernel, (T, KB, NS, DB, r)),
            out_shape=[
                pltpu.VMEM((T, DB), BF16),
                jax.ShapeDtypeStruct((RING, T, KB), BF16),
                jax.ShapeDtypeStruct((CHUNKS, 8, r, K), BF16),
            ],
            in_specs=[any_spec] * 4,
            out_specs=[pl.BlockSpec(memory_space=pltpu.VMEM), any_spec, any_spec],
            scratch_shapes=[
                pltpu.VMEM((K, NS), BF16),
                pltpu.VMEM((NB, DB), BF16),
                pltpu.VMEM((2, 8, r, K), BF16),
                pltpu.VMEM((HSLOTS, 8 * r, NB), BF16),
                pltpu.VMEM((SSLOTS, 4 * r, DB), F32),
                pltpu.VMEM((2, 4 * r, DB), F32),
                pltpu.VMEM((PSLOTS, 4 * r, DB), F32),
                pltpu.VMEM((FSLOTS, 2, r, DB // 2), F32),
                pltpu.VMEM((VSLOTS, 2, r, DB), F32),
                pltpu.VMEM((2, 2, 2 * r, DB // 2), F32),
                pltpu.VMEM((4, 2, r, DB), F32),
                pltpu.VMEM((RING, 1, KB), F32),
                dma, dma,
                dma((5,)), dma((RSLOTS, 2)),
                dma((2,)), dma((2,)),
                dma((4,)), dma((CHUNKS, 2)),
                dma((4,)), dma((CHUNKS,)),
                dma((HSLOTS,)), dma((HSLOTS, 2)), dma((HSLOTS,)),
                dma((2,)), dma((PSLOTS,)),
                dma((SSLOTS,)), dma((FSLOTS,)),
                dma((SSLOTS,)), dma((VSLOTS,)), dma((4,)),
                dma((8,)), dma((2,)), dma,
            ],
            compiler_params=pltpu.CompilerParams(collective_id=0, has_side_effects=True, vmem_limit_bytes=61 * 2**20 + 3 * 2**18),
        )(x_loc, scale_loc.reshape(1, KB), w_in_loc, w_out_loc)
        return outs[0]

    return jax.shard_map(local_block, mesh=mesh, in_specs=(row_spec, P("tp2"), P("tp2", "tp"), P("tp", "tp2")), out_specs=row_spec, check_vma=False)
```
